32 devices in a mesh: qa: 16 (over z, x, core), qb: 2 (over y).
Axes of the slice: x: 2, y: 2, z: 4, core: 2. Of those that a mesh axis runs over, the one named last changes fastest.
Arguments:
- wave_parts: float32 [2, 256, 128, 128], P(None, ('qa', 'qb')), may hold values from -6 to 6
- level_table: float32 [256, 128, 128], P(('qa', 'qb')), may hold values from -2 to 2
- phase_angles: float32 [2, 128], replicated, may hold values from 0.3 to 1.2
Outputs:
- final_parts: float32 [2, 256, 128, 128], P(None, ('qa', 'qb'))
The draws below stay inside these ranges and needn't reach their ends.
All inputs are finite; a program needn't handle non-finite values.
Results may differ from the reference program's by a relative error of at most 0.0003.
Values sent between devices are 32-bit elements; how exact they have to be, the bound alone decides.
No kernel may reach another device: no remote copies, remote signals or barrier semaphores. Data moves between devices by JAX's collectives and lax.ppermute only.
A program may use at most 64 MiB of HBM per device.

```python
import jax
import jax.numpy as jnp
from jax import lax

BLOCKS_DEV = 8
ROWS = 128
LANES = 128
BLOCKS = 256
LAYERS = 2
N_QA = 16
N_QB = 2


def shard_levels(stream_key, dims, cuts, low, top_value):
    def one(position, blocks):
        heights = jax.random.uniform(jax.random.fold_in(jax.random.fold_in(stream_key, 6), position), (blocks,), jnp.float32, low / len(cuts), top_value / len(cuts))
        return jnp.repeat(jnp.exp(heights), dims[position] // blocks).reshape((-1,) + (1,) * (len(dims) - position - 1))

    gain = one(*cuts[0])
    for cut in cuts[1:]:
        gain = gain * one(*cut)
    return gain


def bell_draw(key, dims, width, most, pieces=(), kind=jnp.bfloat16):
    level = shard_levels(key, dims, pieces, -0.22, 0.18) if pieces else 1.0
    result = jax.random.normal(key, dims, jnp.float32) * width * level
    return jnp.minimum(jnp.maximum(result, -most), most).astype(kind)


def setup_inputs(seed: int = 0) -> dict:
    seeds = jax.random.split(jax.random.key(seed), 4)
    wave_parts = bell_draw(seeds[0], (2, BLOCKS, ROWS, LANES), 1.0, 6.0, ((1, 32),), jnp.float32)
    level_table = jnp.clip(jax.random.uniform(seeds[1], (BLOCKS, ROWS, LANES), jnp.float32, -2.0, 2.0) * shard_levels(seeds[1], (BLOCKS, ROWS, LANES), ((0, 32),), -0.4, 0.0), -2.0, 2.0)
    phase_angles = jnp.clip(jax.random.uniform(seeds[2], (LAYERS, LANES), jnp.float32, 0.3, 1.2), 0.3, 1.2)
    return {"wave_parts": wave_parts, "level_table": level_table, "phase_angles": phase_angles}


def count_bits(values, count):
    places = jnp.arange(count.bit_length() - 1, dtype=jnp.int32)
    return jnp.sum((values[..., None] >> places) & 1, axis=-1)


def sign_table(count):
    rank = jnp.arange(count, dtype=jnp.int32)
    parity = count_bits(rank[:, None] & rank[None, :], count) % 2
    real_part = jnp.where(parity == 1, -1.0, 1.0).astype(jnp.float32) * (count ** -0.5)
    return real_part


def turn_dim(values, dim):
    real_part = sign_table(values.shape[dim])
    def times(table):
        moved = jnp.tensordot(values, table, axes=([dim], [0]), precision=lax.Precision.HIGHEST)
        return jnp.moveaxis(moved, -1, dim)
    return times(real_part)


def turn_phase(values, levels, angle):
    turn = angle * levels
    return jnp.stack([values[0] * jnp.cos(turn) + values[1] * jnp.sin(turn), values[1] * jnp.cos(turn) - values[0] * jnp.sin(turn)])


def reference(wave_parts, level_table, phase_angles):
    values = wave_parts
    for layer in range(LAYERS):
        values = turn_phase(values, level_table, phase_angles[layer])
        values = turn_dim(values, 3)
        values = turn_dim(values, 2)
        parts = values.reshape(2, N_QA, N_QB, BLOCKS_DEV, ROWS, LANES)
        parts = turn_dim(parts, 1)
        parts = turn_dim(parts, 2)
        parts = turn_dim(parts, 3)
        values = parts.reshape(values.shape)
    return values
```

```python
import functools

import jax
import jax.numpy as jnp
from jax import lax
from jax.experimental import pallas as pl
from jax.experimental.pallas import tpu as pltpu
from jax.sharding import PartitionSpec as P

COS = (0.99999999952702, -0.49999999256864713, 0.04166664759095227, -0.0013888705067900038,
       2.4793136218611696e-05, -2.735711629719697e-07, 1.8502809653875554e-09)
SIN = (0.9999999999681006, -0.16666666616558576, 0.008333332047516205, -0.00019841145991402124,
       2.75516291724042e-06, -2.4917466240452868e-08, 1.446608995457697e-10)


def poly(coefs, t):
    total = jnp.full_like(t, coefs[-1])
    for c in coefs[-2::-1]:
        total = total * t + c
    return total


def turn(real, imag, levels, angle, scale):
    x = angle * levels
    t = x * x
    c = poly(COS, t) * scale
    s = x * poly(SIN, t) * scale
    return real * c + imag * s, imag * c - real * s


def butterflies(values):
    values = list(values)
    step = 1
    while step < len(values):
        for i in range(len(values)):
            if not i & step:
                u, v = values[i], values[i + step]
                values[i], values[i + step] = u + v, u - v
        step *= 2
    return values


def signs(count, dtype):
    rank = lax.broadcasted_iota(jnp.int32, (count, count), 0) & lax.broadcasted_iota(jnp.int32, (count, count), 1)
    parity = rank
    shift = 1
    while shift < count:
        parity = parity ^ (parity >> shift)
        shift *= 2
    return (1 - 2 * (parity & 1)).astype(dtype)


def split(x, axis):
    high = x.astype(jnp.bfloat16)
    low = (x - high.astype(jnp.float32)).astype(jnp.bfloat16)
    return jnp.concatenate([high, low], axis=axis)


def tile_turn(x, right, left):
    y = jnp.dot(split(x, 1), right, preferred_element_type=jnp.float32)
    return jnp.dot(left, split(y, 0), preferred_element_type=jnp.float32)


def first_kernel(devices, part, scale, wave_ref, level_ref, angle_ref, out_ref):
    tiles = part // 8
    angle = jnp.broadcast_to(angle_ref[0:1, :], (8, wave_ref.shape[2]))

    def step(tile, _):
        for d in range(devices):
            rows = pl.ds(pl.multiple_of(d * part + tile * 8, 8), 8)
            levels = level_ref[rows, :]
            real, imag = turn(wave_ref[0, rows, :], wave_ref[1, rows, :], levels, angle, scale)
            here = pl.ds(pl.multiple_of(tile * 8, 8), 8)
            out_ref[d, 0, here, :] = real
            out_ref[d, 1, here, :] = imag
            out_ref[d, 2, here, :] = levels
        for p in range(2):
            here = pl.ds(pl.multiple_of(tile * 8, 8), 8)
            values = butterflies([out_ref[d, p, here, :] for d in range(devices)])
            for d in range(devices):
                out_ref[d, p, here, :] = values[d]
        return 0

    lax.fori_loop(0, tiles, step, 0)


def middle_kernel(devices, part, scale, in_ref, angle_ref, right_ref, left_ref, out_ref, held):
    lanes = in_ref.shape[3]
    size = left_ref.shape[0]
    per = size // part
    groups = devices // per
    right, left = right_ref[...], left_ref[...]
    for p in range(2):
        for g in range(groups):
            x = in_ref[g * per:(g + 1) * per, p].reshape(size, lanes)
            held[p, g * size:(g + 1) * size] = tile_turn(x, right, left)
    angle = jnp.broadcast_to(angle_ref[1:2, :], (8, lanes))

    def step(tile, _):
        rows = [pl.ds(pl.multiple_of(g * size + tile * 8, 8), 8) for g in range(groups)]
        real = butterflies([held[0, r, :] for r in rows])
        imag = butterflies([held[1, r, :] for r in rows])
        for g in range(groups):
            first = (g * size + tile * 8) // part
            offset = pl.multiple_of((tile * 8) % part, 8)
            levels = in_ref[first, 2, pl.ds(offset, 8), :]
            real[g], imag[g] = turn(real[g], imag[g], levels, angle, scale)
        for p, values in enumerate((real, imag)):
            for r, value in zip(rows, butterflies(values)):
                held[p, r, :] = value
        return 0

    lax.fori_loop(0, size // 8, step, 0)
    for p in range(2):
        for g in range(groups):
            y = tile_turn(held[p, g * size:(g + 1) * size], right, left)
            out_ref[g * per:(g + 1) * per, p] = y.reshape(per, part, lanes)


def last_kernel(devices, part, in_ref, out_ref):
    def step(tile, _):
        for p in range(2):
            here = pl.ds(pl.multiple_of(tile * 8, 8), 8)
            values = butterflies([in_ref[d, p, here, :] for d in range(devices)])
            for d in range(devices):
                rows = pl.ds(pl.multiple_of(d * part + tile * 8, 8), 8)
                out_ref[p, rows, :] = values[d]
        return 0

    lax.fori_loop(0, part // 8, step, 0)


def call(kernel, shape, scratch=()):
    return pl.pallas_call(
        kernel,
        out_shape=jax.ShapeDtypeStruct(shape, jnp.float32),
        scratch_shapes=list(scratch),
    )


def body_fast(axes, devices, wave, levels, angles):
    blocks, rows, lanes = levels.shape
    total = blocks * rows
    part = total // devices
    scale = float(devices * total * lanes) ** -0.5
    wave = wave.reshape(2, total, lanes)
    levels = levels.reshape(total, lanes)
    sent = call(functools.partial(first_kernel, devices, part, scale), (devices, 3, part, lanes))(wave, levels, angles)
    seen = lax.all_to_all(sent, axes, 0, 0, tiled=True)
    sign = signs(lanes, jnp.bfloat16)
    right = jnp.concatenate([sign, sign], axis=0)
    sign = signs(128, jnp.bfloat16)
    left = jnp.concatenate([sign, sign], axis=1)
    back = call(
        functools.partial(middle_kernel, devices, part, scale), (devices, 2, part, lanes),
        [pltpu.VMEM((2, total, lanes), jnp.float32)],
    )(seen, angles, right, left)
    back = lax.all_to_all(back, axes, 0, 0, tiled=True)
    out = call(functools.partial(last_kernel, devices, part), (2, total, lanes))(back)
    return out.reshape(2, blocks, rows, lanes)


def walsh(values, dim):
    count = values.shape[dim]
    moved = jnp.tensordot(values, signs(count, jnp.float32), axes=([dim], [0]), precision=lax.Precision.HIGHEST)
    return jnp.moveaxis(moved, -1, dim) * count ** -0.5


def body_plain(axes, devices, wave, levels, angles):
    blocks, rows, lanes = levels.shape
    part = blocks * rows // devices
    values = wave.reshape(2, devices, part, lanes)
    levels = levels.reshape(devices, part, lanes)
    x = angles[0] * levels
    c, s = jnp.cos(x), jnp.sin(x)
    values = jnp.stack([values[0] * c + values[1] * s, values[1] * c - values[0] * s], axis=1)
    values = walsh(values, 0)
    values = lax.all_to_all(values, axes, 0, 0, tiled=True)
    levels = lax.all_to_all(levels, axes, 0, 0, tiled=True)
    for dim in (0, 2, 3):
        values = walsh(values, dim)
    x = angles[1] * levels
    c, s = jnp.cos(x), jnp.sin(x)
    values = jnp.stack([values[:, 0] * c + values[:, 1] * s, values[:, 1] * c - values[:, 0] * s], axis=1)
    for dim in (0, 2, 3):
        values = walsh(values, dim)
    values = lax.all_to_all(values, axes, 0, 0, tiled=True)
    values = walsh(values, 0)
    return jnp.moveaxis(values, 1, 0).reshape(wave.shape)


def solution(mesh):
    axes = ("qa", "qb")
    devices = mesh.shape["qa"] * mesh.shape["qb"]

    def body(wave, levels, angles):
        total = levels.shape[0] * levels.shape[1]
        part = total // devices
        fast = part % 8 == 0 and 128 % part == 0 and total % 128 == 0
        return (body_fast if fast else body_plain)(axes, devices, wave, levels, angles)

    in_specs = (P(None, axes, None, None), P(axes, None, None), P())
    return jax.shard_map(body, mesh=mesh, in_specs=in_specs, out_specs=in_specs[0], check_vma=False)
```

```python
import functools

import jax
import jax.numpy as jnp
from jax import lax
from jax.experimental import pallas as pl
from jax.experimental.pallas import tpu as pltpu
from jax.sharding import PartitionSpec as P


COS = (0.99999999952702, -0.49999999256864713, 0.04166664759095227, -0.0013888705067900038,
       2.4793136218611696e-05, -2.735711629719697e-07, 1.8502809653875554e-09)
SIN = (0.9999999999681006, -0.16666666616558576, 0.008333332047516205, -0.00019841145991402124,
       2.75516291724042e-06, -2.4917466240452868e-08, 1.446608995457697e-10)


def poly(coefs, t):
    total = jnp.full_like(t, coefs[-1])
    for c in coefs[-2::-1]:
        total = total * t + c
    return total


def turn(real, imag, levels, angle, scale):
    x = angle * levels
    t = x * x
    c = poly(COS, t) * scale
    s = x * poly(SIN, t) * scale
    return real * c + imag * s, imag * c - real * s


def butterflies(values):
    values = list(values)
    step = 1
    while step < len(values):
        for i in range(len(values)):
            if not i & step:
                u, v = values[i], values[i + step]
                values[i], values[i + step] = u + v, u - v
        step *= 2
    return values


def signs(count, dtype):
    rank = lax.broadcasted_iota(jnp.int32, (count, count), 0) & lax.broadcasted_iota(jnp.int32, (count, count), 1)
    parity = rank
    shift = 1
    while shift < count:
        parity = parity ^ (parity >> shift)
        shift *= 2
    return (1 - 2 * (parity & 1)).astype(dtype)


def split(x, axis):
    high = x.astype(jnp.bfloat16)
    low = (x - high.astype(jnp.float32)).astype(jnp.bfloat16)
    return jnp.concatenate([high, low], axis=axis)


def tile_turn(x, right, left):
    y = jnp.dot(split(x, 1), right, preferred_element_type=jnp.float32)
    return jnp.dot(left, split(y, 0), preferred_element_type=jnp.float32)


def first_kernel(devices, group, scale, wave_ref, level_ref, angle_ref, out_ref):
    part, lanes = wave_ref.shape[2:]
    angle = jnp.broadcast_to(angle_ref[0:1, :], (8, lanes))
    tiles = part // 8

    def inner(i, _):
        base, rows = i // tiles * group, pl.ds(pl.multiple_of(i % tiles * 8, 8), 8)
        pairs = [
            turn(wave_ref[0, base + k, rows, :], wave_ref[1, base + k, rows, :], level_ref[base + k, rows, :], angle, scale)
            for k in range(group)
        ]
        for p in range(2):
            for k, value in enumerate(butterflies([pair[p] for pair in pairs])):
                out_ref[base + k, p, rows, :] = value
        return 0

    lax.fori_loop(0, devices // group * tiles, inner, 0, unroll=True)

    def outer(k, _):
        for p in range(2):
            for tile in range(tiles):
                rows = slice(tile * 8, tile * 8 + 8)
                values = butterflies([out_ref[g * group + k, p, rows, :] for g in range(devices // group)])
                for g, value in enumerate(values):
                    out_ref[g * group + k, p, rows, :] = value
        return 0

    lax.fori_loop(0, group, outer, 0, unroll=True)


def pick_kernel(slabs, size, place_ref, wave_ref, level_ref, angle_ref, *refs):
    outs, sems = refs[:-1], refs[-1]
    mine = place_ref[0] // size
    pairs = [(level_ref.at[pl.ds((mine ^ m) * size, size)], outs[m + 2]) for m in range(1, slabs)]
    pairs += [(wave_ref, outs[0]), (level_ref, outs[1]), (angle_ref, outs[2])]
    copies = [pltpu.make_async_copy(*pair, sems.at[k]) for k, pair in enumerate(pairs)]
    for copy in copies:
        copy.start()
    for copy in copies:
        copy.wait()


def deal_kernel(slabs, size, place_ref, level_ref, *refs):
    mine = place_ref[0] % size
    for k in range(size):
        refs[slabs - 1 + k][0] = level_ref[place_ref[0] ^ k]
        for m in range(1, slabs):
            refs[slabs - 1 + k][m] = refs[m - 1][mine ^ k]


def middle_kernel(devices, part, scale, slabs, place_ref, in_ref, angle_ref, right_ref, left_ref, *refs):
    size = devices // slabs
    level_refs, out_ref, held, levels = refs[:size], refs[size], refs[size + 1], refs[size + 2]
    lanes = in_ref.shape[3]
    block = left_ref.shape[0]
    per = block // part
    groups = devices // per
    right, left = right_ref[...], left_ref[...]
    for k in range(size):
        for m in range(slabs):
            levels[pl.ds((place_ref[0] ^ (m * size + k)) * part, part), :] = level_refs[k][m]
    for p in range(2):
        for g in range(groups):
            x = in_ref[g * per:(g + 1) * per, p].reshape(block, lanes)
            held[p, g * block:(g + 1) * block] = tile_turn(x, right, left)
    angle = jnp.broadcast_to(angle_ref[1:2, :], (8, lanes))

    def step(tile, _):
        rows = [pl.ds(pl.multiple_of(g * block + tile * 8, 8), 8) for g in range(groups)]
        real = butterflies([held[0, r, :] for r in rows])
        imag = butterflies([held[1, r, :] for r in rows])
        for g in range(groups):
            real[g], imag[g] = turn(real[g], imag[g], levels[rows[g], :], angle, scale)
        for p, values in enumerate((real, imag)):
            for r, value in zip(rows, butterflies(values)):
                held[p, r, :] = value
        return 0

    lax.fori_loop(0, block // 8, step, 0)
    for p in range(2):
        for g in range(groups):
            y = tile_turn(held[p, g * block:(g + 1) * block], right, left)
            out_ref[g * per:(g + 1) * per, p] = y.reshape(per, part, lanes)


def last_kernel(devices, part, in_ref, out_ref):
    def step(tile, _):
        for p in range(2):
            here = pl.ds(pl.multiple_of(tile * 8, 8), 8)
            values = butterflies([in_ref[d, p, here, :] for d in range(devices)])
            for d in range(devices):
                rows = pl.ds(pl.multiple_of(d * part + tile * 8, 8), 8)
                out_ref[p, rows, :] = values[d]
        return 0

    lax.fori_loop(0, part // 8, step, 0)


def near(x):
    return pltpu.with_memory_space_constraint(x, pltpu.VMEM)


def far(x):
    return pltpu.with_memory_space_constraint(x, pltpu.HBM)


def flat(*shape):
    return jax.ShapeDtypeStruct(shape, jnp.float32)


def swap(x, axes, devices, mask):
    return lax.ppermute(x, axes, [(i, i ^ mask) for i in range(devices)])


PARAMS = pltpu.CompilerParams(vmem_limit_bytes=16 * 2**20)
SCALAR = pl.BlockSpec(memory_space=pltpu.SMEM)
WHOLE = pl.BlockSpec(memory_space=pltpu.VMEM)


def body_fast(axes, devices, slabs, wave, levels, angles):
    blocks, rows, lanes = levels.shape
    total = blocks * rows
    part = total // devices
    size = devices // slabs
    scale = float(devices * total * lanes) ** -0.5
    place = lax.axis_index(axes).astype(jnp.int32).reshape(1)
    wave = wave.reshape(2, devices, part, lanes)
    levels = levels.reshape(devices, part, lanes)
    wave, levels, angles, *picked = pl.pallas_call(
        functools.partial(pick_kernel, slabs, size),
        in_specs=[SCALAR] + [pl.BlockSpec(memory_space=pltpu.HBM)] * 3,
        out_specs=[WHOLE] * (slabs + 2),
        out_shape=[pltpu.VMEM(x.shape, jnp.float32) for x in (wave, levels, angles)]
        + [pltpu.VMEM((size, part, lanes), jnp.float32)] * (slabs - 1),
        scratch_shapes=[pltpu.SemaphoreType.DMA((slabs + 2,))],
        name="pick",
        compiler_params=PARAMS,
    )(place, far(wave), far(levels), far(angles))
    mine = []
    for m in range(1, slabs):
        mine.append(swap(picked[m - 1], axes, devices, m * size))
    sent = pl.pallas_call(
        functools.partial(first_kernel, devices, size, scale),
        in_specs=[WHOLE] * 3,
        out_specs=WHOLE,
        out_shape=flat(devices, 2, part, lanes),
        name="first",
        compiler_params=PARAMS,
    )(near(wave), near(levels), near(angles))
    seen = lax.all_to_all(sent, axes, 0, 0, tiled=True)
    dealt = pl.pallas_call(
        functools.partial(deal_kernel, slabs, size),
        in_specs=[SCALAR] + [WHOLE] * slabs,
        out_specs=[WHOLE] * size,
        out_shape=[pltpu.VMEM((slabs, part, lanes), jnp.float32)] * size,
        name="deal",
        compiler_params=PARAMS,
    )(place, near(levels), *map(near, mine))
    dealt = [dealt[0]] + [swap(dealt[k], axes, devices, k) for k in range(1, size)]
    sign = signs(lanes, jnp.bfloat16)
    right = jnp.concatenate([sign, sign], axis=0)
    sign = signs(128, jnp.bfloat16)
    left = jnp.concatenate([sign, sign], axis=1)
    back = pl.pallas_call(
        functools.partial(middle_kernel, devices, part, scale, slabs),
        in_specs=[SCALAR] + [WHOLE] * (4 + size),
        out_specs=WHOLE,
        out_shape=pltpu.VMEM((devices, 2, part, lanes), jnp.float32),
        scratch_shapes=[pltpu.VMEM((2, total, lanes), jnp.float32), pltpu.VMEM((total, lanes), jnp.float32)],
        name="middle",
        compiler_params=PARAMS,
    )(place, near(seen), near(angles), right, left, *map(near, dealt))
    back = lax.all_to_all(back, axes, 0, 0, tiled=True)
    out = pl.pallas_call(
        functools.partial(last_kernel, devices, part),
        in_specs=[WHOLE],
        out_specs=WHOLE,
        out_shape=flat(2, total, lanes),
        name="last",
        compiler_params=PARAMS,
    )(near(back))
    return out.reshape(2, blocks, rows, lanes)


def walsh(values, dim):
    count = values.shape[dim]
    moved = jnp.tensordot(values, signs(count, jnp.float32), axes=([dim], [0]), precision=lax.Precision.HIGHEST)
    return jnp.moveaxis(moved, -1, dim) * count ** -0.5


def body_plain(axes, devices, wave, levels, angles):
    blocks, rows, lanes = levels.shape
    part = blocks * rows // devices
    values = wave.reshape(2, devices, part, lanes)
    levels = levels.reshape(devices, part, lanes)
    x = angles[0] * levels
    c, s = jnp.cos(x), jnp.sin(x)
    values = jnp.stack([values[0] * c + values[1] * s, values[1] * c - values[0] * s], axis=1)
    values = walsh(values, 0)
    values = lax.all_to_all(values, axes, 0, 0, tiled=True)
    levels = lax.all_to_all(levels, axes, 0, 0, tiled=True)
    for dim in (0, 2, 3):
        values = walsh(values, dim)
    x = angles[1] * levels
    c, s = jnp.cos(x), jnp.sin(x)
    values = jnp.stack([values[:, 0] * c + values[:, 1] * s, values[:, 1] * c - values[:, 0] * s], axis=1)
    for dim in (0, 2, 3):
        values = walsh(values, dim)
    values = lax.all_to_all(values, axes, 0, 0, tiled=True)
    values = walsh(values, 0)
    return jnp.moveaxis(values, 1, 0).reshape(wave.shape)


def solution(mesh):
    axes = ("qa", "qb")
    devices = mesh.shape["qa"] * mesh.shape["qb"]

    def body(wave, levels, angles):
        total = levels.shape[0] * levels.shape[1]
        part = total // devices
        fast = part % 8 == 0 and 128 % part == 0 and total % 128 == 0
        slabs = mesh.shape["qa"] // 4
        if fast and slabs > 1:
            return body_fast(axes, devices, slabs, wave, levels, angles)
        return body_plain(axes, devices, wave, levels, angles)

    in_specs = (P(None, axes, None, None), P(axes, None, None), P())
    return jax.shard_map(body, mesh=mesh, in_specs=in_specs, out_specs=in_specs[0], check_vma=False)
```

```python
import functools

import jax
import jax.numpy as jnp
from jax import lax
from jax.experimental import pallas as pl
from jax.experimental.pallas import tpu as pltpu
from jax.sharding import PartitionSpec as P


COS = (0.99999999952702, -0.49999999256864713, 0.04166664759095227, -0.0013888705067900038,
       2.4793136218611696e-05, -2.735711629719697e-07, 1.8502809653875554e-09)
SIN = (0.9999999999681006, -0.16666666616558576, 0.008333332047516205, -0.00019841145991402124,
       2.75516291724042e-06, -2.4917466240452868e-08, 1.446608995457697e-10)


def poly(coefs, t):
    total = jnp.full_like(t, coefs[-1])
    for c in coefs[-2::-1]:
        total = total * t + c
    return total


def butterflies(values):
    values = list(values)
    step = 1
    while step < len(values):
        for i in range(len(values)):
            if not i & step:
                u, v = values[i], values[i + step]
                values[i], values[i + step] = u + v, u - v
        step *= 2
    return values


def signs(count, dtype):
    rank = lax.broadcasted_iota(jnp.int32, (count, count), 0) & lax.broadcasted_iota(jnp.int32, (count, count), 1)
    parity = rank
    shift = 1
    while shift < count:
        parity = parity ^ (parity >> shift)
        shift *= 2
    return (1 - 2 * (parity & 1)).astype(dtype)


def split(x, axis):
    high = x.astype(jnp.bfloat16)
    low = (x - high.astype(jnp.float32)).astype(jnp.bfloat16)
    return jnp.concatenate([high, low], axis=axis)


def tile_turn(x, right, left):
    y = jnp.dot(split(x, 1), right, preferred_element_type=jnp.float32)
    return jnp.dot(left, split(y, 0), preferred_element_type=jnp.float32)


def trig(x, scale):
    t = x * x
    return poly(COS, t) * scale, x * poly(SIN, t) * scale


def rotate(real, imag, c, s):
    return real * c + imag * s, imag * c - real * s


def pick_kernel(slabs, size, place_ref, wave_ref, level_ref, angle_ref, *refs):
    outs, sems = refs[:-1], refs[-1]
    mine = place_ref[0] // size
    pairs = list(zip((wave_ref, level_ref, angle_ref), outs))
    pairs += [(level_ref.at[pl.ds((mine ^ m) * size, size)], outs[m + 2]) for m in range(1, slabs)]
    copies = [pltpu.make_async_copy(*pair, sems.at[k]) for k, pair in enumerate(pairs)]
    for copy in copies:
        copy.start()
    for copy in copies:
        copy.wait()


def first_kernel(devices, part, scale, wave_ref, level_ref, angle_ref, right_ref, left_ref, out_ref, held):
    lanes = wave_ref.shape[2]
    block = left_ref.shape[0]
    groups, per = devices * part // block, block // part
    right, left = right_ref[...], left_ref[...]
    angle = jnp.broadcast_to(angle_ref[0:1, :], (block, lanes))
    for g in range(groups):
        rows = slice(g * block, (g + 1) * block)
        c, s = trig(angle * level_ref[rows, :], scale)
        for p, x in enumerate(rotate(wave_ref[0, rows, :], wave_ref[1, rows, :], c, s)):
            held[p, rows, :] = tile_turn(x, right, left)
    for p in range(2):
        for tile in range(block // 8):
            values = butterflies([held[p, g * block + tile * 8:g * block + tile * 8 + 8, :] for g in range(groups)])
            k, row = tile * 8 // part, tile * 8 % part
            for g, value in enumerate(values):
                out_ref[g * per + k, p, row:row + 8, :] = value


def deal_kernel(slabs, size, place_ref, *refs):
    mine = place_ref[0] % size
    for k in range(size):
        for m in range(slabs):
            refs[slabs + k][m] = refs[m][mine ^ k]


def trig_kernel(slabs, size, scale, place_ref, angle_ref, *refs):
    level_refs, cos_ref, sin_ref = refs[:size], refs[size], refs[size + 1]
    angle = jnp.broadcast_to(angle_ref[1:2, :], cos_ref.shape[1:])
    for k in range(size):
        for m in range(slabs):
            whose = place_ref[0] ^ (m * size + k)
            cos_ref[whose], sin_ref[whose] = trig(angle * level_refs[k][m], scale)


def turn_devices(slabs, size, tiles, seen_ref, cos_ref, sin_ref, held):
    for tile in tiles:
        rows = slice(tile * 8, tile * 8 + 8)
        for z in range(slabs):
            for p in range(2):
                values = butterflies([seen_ref[z * size + q, p, rows, :] for q in range(size)])
                for q, value in enumerate(values):
                    held[z * size + q, p, rows, :] = value
        for q in range(size):
            real, imag = (butterflies([held[z * size + q, p, rows, :] for z in range(slabs)]) for p in range(2))
            for z in range(slabs):
                d = z * size + q
                real[z], imag[z] = rotate(real[z], imag[z], cos_ref[d, rows, :], sin_ref[d, rows, :])
            for p, values in enumerate((real, imag)):
                for z, value in enumerate(butterflies(values)):
                    held[z * size + q, p, rows, :] = value


def few_kernel(slabs, size, place_ref, seen_ref, cos_ref, sin_ref, *refs):
    outs, held = refs[:slabs], refs[slabs]
    count = outs[0].shape[2] // 8
    turn_devices(slabs, size, range(count), seen_ref, cos_ref, sin_ref, held)
    mine = place_ref[0] // size
    for m in range(slabs):
        for p in range(2):
            for tile in range(count):
                rows = slice(tile * 8, tile * 8 + 8)
                values = butterflies([held[(mine ^ m) * size + q, p, rows, :] for q in range(size)])
                for q, value in enumerate(values):
                    outs[m][q, p, rows, :] = value


def most_kernel(slabs, size, seen_ref, cos_ref, sin_ref, right_ref, left_ref, out_ref, held):
    part, lanes = seen_ref.shape[2:]
    devices = slabs * size
    start = (part - out_ref.shape[2]) // 8
    turn_devices(slabs, size, range(start, part // 8), seen_ref, cos_ref, sin_ref, held)
    right, left = right_ref[...], left_ref[...]
    step = left.shape[0] // 8
    for tile in range(start, part // 8):
        rows = slice(tile * 8, tile * 8 + 8)
        for p in range(2):
            for z in range(slabs):
                values = butterflies([held[z * size + q, p, rows, :] for q in range(size)])
                for q, value in enumerate(values):
                    held[z * size + q, p, rows, :] = value
            for d in range(0, devices, step):
                x = held[d:d + step, p, rows, :].reshape(step * 8, lanes)
                out_ref[d:d + step, p, (tile - start) * 8:(tile - start) * 8 + 8, :] = tile_turn(x, right, left).reshape(step, 8, lanes)


def gather_kernel(slabs, size, place_ref, right_ref, left_ref, *refs):
    parts, out_ref, held = refs[:size], refs[size], refs[size + 1]
    for k in range(size):
        for m in range(slabs):
            held[place_ref[0] ^ (m * size + k)] = parts[k][m]
    right, left = right_ref[...], left_ref[...]
    step = left.shape[0] // 8
    for p in range(2):
        for d in range(0, slabs * size, step):
            for row in range(0, held.shape[2], 8):
                x = held[d:d + step, p, row:row + 8, :].reshape(step * 8, held.shape[3])
                out_ref[d:d + step, p, row:row + 8, :] = tile_turn(x, right, left).reshape(step, 8, held.shape[3])


def last_kernel(devices, part, few_ref, most_ref, out_ref, held, done, sems):
    tiles = part // 8
    low = 4
    high = devices // low

    start = few_ref.shape[2] // 8

    def source(d, p, tile):
        ref, row = (few_ref, tile * 8) if tile < start else (most_ref, (tile - start) * 8)
        return ref[d, p, row:row + 8, :]

    copies = []
    for p in range(2):
        for k in range(low):
            for tile in range(tiles):
                values = butterflies([source(h * low + k, p, tile) for h in range(high)])
                for h, value in enumerate(values):
                    held[p, h, k * tiles + tile] = value
        for h in range(high):
            values = butterflies([held[p, h, i] for i in range(low * tiles)])
            for i, value in enumerate(values):
                done[p, (h * low * tiles + i) * 8:(h * low * tiles + i) * 8 + 8, :] = value
            rows = pl.ds(h * low * part, low * part)
            copies.append(pltpu.make_async_copy(done.at[p, rows], out_ref.at[p, rows], sems.at[p * high + h]))
            copies[-1].start()
    for copy in copies:
        copy.wait()


def near(x):
    return pltpu.with_memory_space_constraint(x, pltpu.VMEM)


def far(x):
    return pltpu.with_memory_space_constraint(x, pltpu.HBM)


def flat(*shape):
    return jax.ShapeDtypeStruct(shape, jnp.float32)


def held_shape(*shape):
    return pltpu.VMEM(shape, jnp.float32)


def swap(x, axes, devices, mask):
    return lax.ppermute(x, axes, [(i, i ^ mask) for i in range(devices)])


FEW = 16
PARAMS = pltpu.CompilerParams(vmem_limit_bytes=16 * 2**20)
SCALAR = pl.BlockSpec(memory_space=pltpu.SMEM)
WHOLE = pl.BlockSpec(memory_space=pltpu.VMEM)
FAR = pl.BlockSpec(memory_space=pltpu.HBM)


def kernel_call(kernel, in_specs, out_shape, scratch=(), out_specs=None):
    count = len(out_shape) if isinstance(out_shape, list) else 0
    return pl.pallas_call(
        kernel,
        in_specs=in_specs,
        out_specs=out_specs or ([WHOLE] * count if count else WHOLE),
        out_shape=out_shape,
        scratch_shapes=list(scratch),
        compiler_params=PARAMS,
    )


def body_fast(axes, devices, slabs, wave, levels, angles):
    blocks, rows, lanes = levels.shape
    total = blocks * rows
    part = total // devices
    size = devices // slabs
    count = FEW
    scale = float(devices * total * lanes) ** -0.5
    place = lax.axis_index(axes).astype(jnp.int32).reshape(1)
    wave = wave.reshape(2, total, lanes)
    levels = levels.reshape(devices, part, lanes)
    sign = signs(lanes, jnp.bfloat16)
    right = jnp.concatenate([sign, sign], axis=0)
    full = signs(128, jnp.bfloat16)
    rank = jnp.arange(128)
    small = jnp.where(rank[:, None] // 8 == rank[None, :] // 8, jnp.tile(signs(8, jnp.bfloat16), (16, 16)), 0)
    left = jnp.concatenate([full, full], axis=1)
    left_small = jnp.concatenate([small, small], axis=1)

    wave, levels, angles, *picked = kernel_call(
        functools.partial(pick_kernel, slabs, size), [SCALAR] + [FAR] * 3,
        [held_shape(*x.shape) for x in (wave, levels, angles)] + [held_shape(size, part, lanes)] * (slabs - 1),
        [pltpu.SemaphoreType.DMA((slabs + 2,))],
    )(place, far(wave), far(levels), far(angles))
    own = lax.dynamic_slice_in_dim(levels, place[0] // size * size, size, 0)
    mine = [own]
    for m in range(1, slabs):
        mine.append(swap(picked[m - 1], axes, devices, m * size))
    sent = kernel_call(
        functools.partial(first_kernel, devices, part, scale), [WHOLE] * 5,
        flat(devices, 2, part, lanes), [held_shape(2, total, lanes)],
    )(near(wave), near(levels.reshape(total, lanes)), near(angles), right, left)
    seen = lax.all_to_all(sent, axes, 0, 0, tiled=True)
    dealt = kernel_call(
        functools.partial(deal_kernel, slabs, size), [SCALAR] + [WHOLE] * slabs,
        [held_shape(slabs, part, lanes)] * size,
    )(place, *map(near, mine))
    dealt = [dealt[0]] + [swap(dealt[k], axes, devices, k) for k in range(1, size)]
    cos, sin = kernel_call(
        functools.partial(trig_kernel, slabs, size, scale), [SCALAR] + [WHOLE] * (1 + size),
        [held_shape(devices, part, lanes)] * 2,
    )(place, near(angles), *map(near, dealt))

    seen = near(seen)
    few = kernel_call(
        functools.partial(few_kernel, slabs, size), [SCALAR] + [WHOLE] * 3,
        [held_shape(size, 2, count, lanes)] * slabs, [held_shape(devices, 2, count, lanes)],
    )(place, seen, cos, sin)
    few = [few[0], *few[1:]]
    for m in range(1, slabs):
        few[m] = swap(few[m], axes, devices, m * size)
    most = kernel_call(
        functools.partial(most_kernel, slabs, size), [WHOLE] * 5,
        flat(devices, 2, part - count, lanes), [held_shape(devices, 2, part, lanes)],
    )(seen, cos, sin, right, left_small)
    most = lax.all_to_all(most, axes, 0, 0, tiled=True)
    few = kernel_call(
        functools.partial(deal_kernel, slabs, size), [SCALAR] + [WHOLE] * slabs,
        [held_shape(slabs, 2, count, lanes)] * size,
    )(place, *map(near, few))
    few = [few[0]] + [swap(few[k], axes, devices, k) for k in range(1, size)]
    few = kernel_call(
        functools.partial(gather_kernel, slabs, size), [SCALAR] + [WHOLE] * (2 + size),
        held_shape(devices, 2, count, lanes), [held_shape(devices, 2, count, lanes)],
    )(place, right, left_small, *map(near, few))
    out = kernel_call(
        functools.partial(last_kernel, devices, part), [WHOLE] * 2, flat(2, total, lanes),
        [held_shape(2, devices // 4, part // 2, 8, lanes), held_shape(2, total, lanes), pltpu.SemaphoreType.DMA((devices // 2,))],
        FAR,
    )(near(few), near(most))
    return out.reshape(2, blocks, rows, lanes)


def walsh(values, dim):
    count = values.shape[dim]
    moved = jnp.tensordot(values, signs(count, jnp.float32), axes=([dim], [0]), precision=lax.Precision.HIGHEST)
    return jnp.moveaxis(moved, -1, dim) * count ** -0.5


def body_plain(axes, devices, wave, levels, angles):
    blocks, rows, lanes = levels.shape
    part = blocks * rows // devices
    values = wave.reshape(2, devices, part, lanes)
    levels = levels.reshape(devices, part, lanes)
    x = angles[0] * levels
    c, s = jnp.cos(x), jnp.sin(x)
    values = jnp.stack([values[0] * c + values[1] * s, values[1] * c - values[0] * s], axis=1)
    values = walsh(values, 0)
    values = lax.all_to_all(values, axes, 0, 0, tiled=True)
    levels = lax.all_to_all(levels, axes, 0, 0, tiled=True)
    for dim in (0, 2, 3):
        values = walsh(values, dim)
    x = angles[1] * levels
    c, s = jnp.cos(x), jnp.sin(x)
    values = jnp.stack([values[:, 0] * c + values[:, 1] * s, values[:, 1] * c - values[:, 0] * s], axis=1)
    for dim in (0, 2, 3):
        values = walsh(values, dim)
    values = lax.all_to_all(values, axes, 0, 0, tiled=True)
    values = walsh(values, 0)
    return jnp.moveaxis(values, 1, 0).reshape(wave.shape)


def solution(mesh):
    axes = ("qa", "qb")
    devices = mesh.shape["qa"] * mesh.shape["qb"]

    def body(wave, levels, angles):
        total = levels.shape[0] * levels.shape[1]
        part = total // devices
        fast = part % 16 == 0 and 128 % part == 0 and total % 128 == 0 and devices % 16 == 0
        slabs = mesh.shape["qa"] // 4
        if fast and slabs > 1:
            return body_fast(axes, devices, slabs, wave, levels, angles)
        return body_plain(axes, devices, wave, levels, angles)

    in_specs = (P(None, axes, None, None), P(axes, None, None), P())
    return jax.shard_map(body, mesh=mesh, in_specs=in_specs, out_specs=in_specs[0], check_vma=False)
```

```python
import functools

import jax
import jax.numpy as jnp
from jax import lax
from jax.experimental import pallas as pl
from jax.experimental.pallas import tpu as pltpu
from jax.sharding import PartitionSpec as P


COS = (0.99999999952702, -0.49999999256864713, 0.04166664759095227, -0.0013888705067900038,
       2.4793136218611696e-05, -2.735711629719697e-07, 1.8502809653875554e-09)
SIN = (0.9999999999681006, -0.16666666616558576, 0.008333332047516205, -0.00019841145991402124,
       2.75516291724042e-06, -2.4917466240452868e-08, 1.446608995457697e-10)


def poly(coefs, t):
    total = jnp.full_like(t, coefs[-1])
    for c in coefs[-2::-1]:
        total = total * t + c
    return total


def butterflies(values):
    values = list(values)
    step = 1
    while step < len(values):
        for i in range(len(values)):
            if not i & step:
                u, v = values[i], values[i + step]
                values[i], values[i + step] = u + v, u - v
        step *= 2
    return values


def signs(count, dtype):
    rank = lax.broadcasted_iota(jnp.int32, (count, count), 0) & lax.broadcasted_iota(jnp.int32, (count, count), 1)
    parity = rank
    shift = 1
    while shift < count:
        parity = parity ^ (parity >> shift)
        shift *= 2
    return (1 - 2 * (parity & 1)).astype(dtype)


def split(x, axis):
    high = x.astype(jnp.bfloat16)
    low = (x - high.astype(jnp.float32)).astype(jnp.bfloat16)
    return jnp.concatenate([high, low], axis=axis)


def tile_turn(x, right, left):
    y = jnp.dot(split(x, 1), right, preferred_element_type=jnp.float32)
    return jnp.dot(left, split(y, 0), preferred_element_type=jnp.float32)


def trig(x, scale):
    t = x * x
    return poly(COS, t) * scale, x * poly(SIN, t) * scale


def rotate(real, imag, c, s):
    return real * c + imag * s, imag * c - real * s


def pick_kernel(slabs, size, place_ref, wave_ref, level_ref, angle_ref, *refs):
    outs, sems = refs[:-1], refs[-1]
    mine = place_ref[0] // size
    pairs = list(zip((wave_ref, level_ref, angle_ref), outs))
    pairs += [(level_ref.at[pl.ds((mine ^ m) * size, size)], outs[m + 2]) for m in range(1, slabs)]
    copies = [pltpu.make_async_copy(*pair, sems.at[k]) for k, pair in enumerate(pairs)]
    for copy in copies:
        copy.start()
    for copy in copies:
        copy.wait()


def first_kernel(slots, part, scale, wave_ref, level_ref, angle_ref, right_ref, left_ref, out_ref, held):
    lanes = wave_ref.shape[2]
    block = left_ref.shape[0]
    groups, per = len(slots) * part // block, block // part
    right, left = right_ref[...], left_ref[...]
    angle = jnp.broadcast_to(angle_ref[0:1, :], (block, lanes))
    for g in range(groups):
        rows = slice(g * block, (g + 1) * block)
        c, s = trig(angle * level_ref[rows, :], scale)
        for p, x in enumerate(rotate(wave_ref[0, rows, :], wave_ref[1, rows, :], c, s)):
            held[p, rows, :] = tile_turn(x, right, left)
    for p in range(2):
        for tile in range(block // 8):
            values = butterflies([held[p, g * block + tile * 8:g * block + tile * 8 + 8, :] for g in range(groups)])
            k, row = tile * 8 // part, tile * 8 % part
            for g, value in enumerate(values):
                out_ref[slots[g * per + k], p, row:row + 8, :] = value


def deal_kernel(slabs, size, place_ref, *refs):
    mine = place_ref[0] % size
    for k in range(size):
        for m in range(slabs):
            refs[slabs + k][m] = refs[m][mine ^ k]


def trig_kernel(slabs, size, scale, place_ref, angle_ref, *refs):
    level_refs, cos_ref, sin_ref = refs[:size], refs[size], refs[size + 1]
    angle = jnp.broadcast_to(angle_ref[1:2, :], cos_ref.shape[1:])
    for k in range(size):
        for m in range(slabs):
            whose = place_ref[0] ^ (m * size + k)
            cos_ref[whose], sin_ref[whose] = trig(angle * level_refs[k][m], scale)


def turn_devices(slabs, size, slots, tiles, seen_ref, cos_ref, sin_ref, held):
    for tile in tiles:
        rows = slice(tile * 8, tile * 8 + 8)
        for z in range(slabs):
            for p in range(2):
                values = butterflies([seen_ref[slots[z * size + q], p, rows, :] for q in range(size)])
                for q, value in enumerate(values):
                    held[z * size + q, p, rows, :] = value
        for q in range(size):
            real, imag = (butterflies([held[z * size + q, p, rows, :] for z in range(slabs)]) for p in range(2))
            for z in range(slabs):
                d = z * size + q
                real[z], imag[z] = rotate(real[z], imag[z], cos_ref[d, rows, :], sin_ref[d, rows, :])
            for p, values in enumerate((real, imag)):
                for z, value in enumerate(butterflies(values)):
                    held[z * size + q, p, rows, :] = value


def few_kernel(slabs, size, slots, place_ref, seen_ref, cos_ref, sin_ref, *refs):
    outs, held = refs[:slabs], refs[slabs]
    count = outs[0].shape[2] // 8
    turn_devices(slabs, size, slots, range(count), seen_ref, cos_ref, sin_ref, held)
    mine = place_ref[0] // size
    for m in range(slabs):
        for p in range(2):
            for tile in range(count):
                rows = slice(tile * 8, tile * 8 + 8)
                values = butterflies([held[(mine ^ m) * size + q, p, rows, :] for q in range(size)])
                for q, value in enumerate(values):
                    outs[m][q, p, rows, :] = value


def most_kernel(slabs, size, slots, seen_ref, cos_ref, sin_ref, right_ref, left_ref, out_ref, held):
    part, lanes = seen_ref.shape[2:]
    devices = slabs * size
    start = (part - out_ref.shape[2]) // 8
    turn_devices(slabs, size, slots, range(start, part // 8), seen_ref, cos_ref, sin_ref, held)
    right, left = right_ref[...], left_ref[...]
    step = left.shape[0] // 8
    for tile in range(start, part // 8):
        rows = slice(tile * 8, tile * 8 + 8)
        for p in range(2):
            for z in range(slabs):
                values = butterflies([held[z * size + q, p, rows, :] for q in range(size)])
                for q, value in enumerate(values):
                    held[z * size + q, p, rows, :] = value
            for d in range(0, devices, step):
                x = held[d:d + step, p, rows, :].reshape(step * 8, lanes)
                out_ref[d:d + step, p, (tile - start) * 8:(tile - start) * 8 + 8, :] = tile_turn(x, right, left).reshape(step, 8, lanes)


def gather_kernel(slabs, size, place_ref, right_ref, left_ref, *refs):
    parts, out_ref, held = refs[:size], refs[size], refs[size + 1]
    for k in range(size):
        for m in range(slabs):
            held[place_ref[0] ^ (m * size + k)] = parts[k][m]
    right, left = right_ref[...], left_ref[...]
    step = left.shape[0] // 8
    for p in range(2):
        for d in range(0, slabs * size, step):
            for row in range(0, held.shape[2], 8):
                x = held[d:d + step, p, row:row + 8, :].reshape(step * 8, held.shape[3])
                out_ref[d:d + step, p, row:row + 8, :] = tile_turn(x, right, left).reshape(step, 8, held.shape[3])


def last_kernel(devices, part, few_ref, most_ref, out_ref, held, done, sems):
    tiles = part // 8
    low = 4
    high = devices // low

    start = few_ref.shape[2] // 8

    def source(d, p, tile):
        ref, row = (few_ref, tile * 8) if tile < start else (most_ref, (tile - start) * 8)
        return ref[d, p, row:row + 8, :]

    copies = []
    for p in range(2):
        for k in range(low):
            for tile in range(tiles):
                values = butterflies([source(h * low + k, p, tile) for h in range(high)])
                for h, value in enumerate(values):
                    held[p, h, k * tiles + tile] = value
        for h in range(high):
            values = butterflies([held[p, h, i] for i in range(low * tiles)])
            for i, value in enumerate(values):
                done[p, (h * low * tiles + i) * 8:(h * low * tiles + i) * 8 + 8, :] = value
            rows = pl.ds(h * low * part, low * part)
            copies.append(pltpu.make_async_copy(done.at[p, rows], out_ref.at[p, rows], sems.at[p * high + h]))
            copies[-1].start()
    for copy in copies:
        copy.wait()


def near(x):
    return pltpu.with_memory_space_constraint(x, pltpu.VMEM)


def far(x):
    return pltpu.with_memory_space_constraint(x, pltpu.HBM)


def flat(*shape):
    return jax.ShapeDtypeStruct(shape, jnp.float32)


def held_shape(*shape):
    return pltpu.VMEM(shape, jnp.float32)


def swap(x, axes, devices, mask):
    return lax.ppermute(x, axes, [(i, i ^ mask) for i in range(devices)])


FEW = 16
PARAMS = pltpu.CompilerParams(vmem_limit_bytes=16 * 2**20)
SCALAR = pl.BlockSpec(memory_space=pltpu.SMEM)
WHOLE = pl.BlockSpec(memory_space=pltpu.VMEM)
FAR = pl.BlockSpec(memory_space=pltpu.HBM)


def device_order(devices, core):
    low, high = core.bit_length() - 1, devices.bit_length() - 1
    bits = [high - 1, *range(low - 1, -1, -1), low + 1, *range(high - 2, low + 1, -1), low]
    order = [sum((rank >> (high - 1 - i) & 1) << bit for i, bit in enumerate(bits)) for rank in range(devices)]
    return order, [order.index(d) for d in range(devices)]


def kernel_call(kernel, in_specs, out_shape, scratch=(), out_specs=None):
    count = len(out_shape) if isinstance(out_shape, list) else 0
    return pl.pallas_call(
        kernel,
        in_specs=in_specs,
        out_specs=out_specs or ([WHOLE] * count if count else WHOLE),
        out_shape=out_shape,
        scratch_shapes=list(scratch),
        compiler_params=PARAMS,
    )


def body_fast(axes, devices, slabs, core, wave, levels, angles):
    blocks, rows, lanes = levels.shape
    total = blocks * rows
    part = total // devices
    size = devices // slabs
    count = FEW
    scale = float(devices * total * lanes) ** -0.5
    order, slots = device_order(devices, core)
    place = lax.axis_index(axes).astype(jnp.int32).reshape(1)
    wave = wave.reshape(2, total, lanes)
    levels = levels.reshape(devices, part, lanes)
    sign = signs(lanes, jnp.bfloat16)
    right = jnp.concatenate([sign, sign], axis=0)
    full = signs(128, jnp.bfloat16)
    rank = jnp.arange(128)
    small = jnp.where(rank[:, None] // 8 == rank[None, :] // 8, jnp.tile(signs(8, jnp.bfloat16), (16, 16)), 0)
    left = jnp.concatenate([full, full], axis=1)
    left_small = jnp.concatenate([small, small], axis=1)

    wave, levels, angles, *picked = kernel_call(
        functools.partial(pick_kernel, slabs, size), [SCALAR] + [FAR] * 3,
        [held_shape(*x.shape) for x in (wave, levels, angles)] + [held_shape(size, part, lanes)] * (slabs - 1),
        [pltpu.SemaphoreType.DMA((slabs + 2,))],
    )(place, far(wave), far(levels), far(angles))
    own = lax.dynamic_slice_in_dim(levels, place[0] // size * size, size, 0)
    mine = [own]
    for m in range(1, slabs):
        mine.append(swap(picked[m - 1], axes, devices, m * size))
    sent = kernel_call(
        functools.partial(first_kernel, slots, part, scale), [WHOLE] * 5,
        flat(devices, 2, part, lanes), [held_shape(2, total, lanes)],
    )(near(wave), near(levels.reshape(total, lanes)), near(angles), right, left)
    seen = lax.all_to_all(sent, axes, 0, 0, tiled=True, axis_index_groups=[order])
    dealt = kernel_call(
        functools.partial(deal_kernel, slabs, size), [SCALAR] + [WHOLE] * slabs,
        [held_shape(slabs, part, lanes)] * size,
    )(place, *map(near, mine))
    dealt = [dealt[0]] + [swap(dealt[k], axes, devices, k) for k in range(1, size)]
    cos, sin = kernel_call(
        functools.partial(trig_kernel, slabs, size, scale), [SCALAR] + [WHOLE] * (1 + size),
        [held_shape(devices, part, lanes)] * 2,
    )(place, near(angles), *map(near, dealt))

    seen = near(seen)
    few = kernel_call(
        functools.partial(few_kernel, slabs, size, slots), [SCALAR] + [WHOLE] * 3,
        [held_shape(size, 2, count, lanes)] * slabs, [held_shape(devices, 2, count, lanes)],
    )(place, seen, cos, sin)
    few = [few[0], *few[1:]]
    for m in range(1, slabs):
        few[m] = swap(few[m], axes, devices, m * size)
    most = kernel_call(
        functools.partial(most_kernel, slabs, size, slots), [WHOLE] * 5,
        flat(devices, 2, part - count, lanes), [held_shape(devices, 2, part, lanes)],
    )(seen, cos, sin, right, left_small)
    most = lax.all_to_all(most, axes, 0, 0, tiled=True)
    few = kernel_call(
        functools.partial(deal_kernel, slabs, size), [SCALAR] + [WHOLE] * slabs,
        [held_shape(slabs, 2, count, lanes)] * size,
    )(place, *map(near, few))
    few = [few[0]] + [swap(few[k], axes, devices, k) for k in range(1, size)]
    few = kernel_call(
        functools.partial(gather_kernel, slabs, size), [SCALAR] + [WHOLE] * (2 + size),
        held_shape(devices, 2, count, lanes), [held_shape(devices, 2, count, lanes)],
    )(place, right, left_small, *map(near, few))
    out = kernel_call(
        functools.partial(last_kernel, devices, part), [WHOLE] * 2, flat(2, total, lanes),
        [held_shape(2, devices // 4, part // 2, 8, lanes), held_shape(2, total, lanes), pltpu.SemaphoreType.DMA((devices // 2,))],
        FAR,
    )(near(few), near(most))
    return out.reshape(2, blocks, rows, lanes)


def walsh(values, dim):
    count = values.shape[dim]
    moved = jnp.tensordot(values, signs(count, jnp.float32), axes=([dim], [0]), precision=lax.Precision.HIGHEST)
    return jnp.moveaxis(moved, -1, dim) * count ** -0.5


def body_plain(axes, devices, wave, levels, angles):
    blocks, rows, lanes = levels.shape
    part = blocks * rows // devices
    values = wave.reshape(2, devices, part, lanes)
    levels = levels.reshape(devices, part, lanes)
    x = angles[0] * levels
    c, s = jnp.cos(x), jnp.sin(x)
    values = jnp.stack([values[0] * c + values[1] * s, values[1] * c - values[0] * s], axis=1)
    values = walsh(values, 0)
    values = lax.all_to_all(values, axes, 0, 0, tiled=True)
    levels = lax.all_to_all(levels, axes, 0, 0, tiled=True)
    for dim in (0, 2, 3):
        values = walsh(values, dim)
    x = angles[1] * levels
    c, s = jnp.cos(x), jnp.sin(x)
    values = jnp.stack([values[:, 0] * c + values[:, 1] * s, values[:, 1] * c - values[:, 0] * s], axis=1)
    for dim in (0, 2, 3):
        values = walsh(values, dim)
    values = lax.all_to_all(values, axes, 0, 0, tiled=True)
    values = walsh(values, 0)
    return jnp.moveaxis(values, 1, 0).reshape(wave.shape)


def solution(mesh):
    axes = ("qa", "qb")
    devices = mesh.shape["qa"] * mesh.shape["qb"]

    def body(wave, levels, angles):
        total = levels.shape[0] * levels.shape[1]
        part = total // devices
        fast = part % 16 == 0 and 128 % part == 0 and total % 128 == 0 and devices % 16 == 0
        slabs = mesh.shape["qa"] // 4
        if fast and slabs > 1:
            return body_fast(axes, devices, slabs, mesh.shape["qb"], wave, levels, angles)
        return body_plain(axes, devices, wave, levels, angles)

    in_specs = (P(None, axes, None, None), P(axes, None, None), P())
    return jax.shard_map(body, mesh=mesh, in_specs=in_specs, out_specs=in_specs[0], check_vma=False)
```

```python
import functools

import jax
import jax.numpy as jnp
from jax import lax
from jax.experimental import pallas as pl
from jax.experimental.pallas import tpu as pltpu
from jax.sharding import PartitionSpec as P


COS = (0.99999999952702, -0.49999999256864713, 0.04166664759095227, -0.0013888705067900038,
       2.4793136218611696e-05, -2.735711629719697e-07, 1.8502809653875554e-09)
SIN = (0.9999999999681006, -0.16666666616558576, 0.008333332047516205, -0.00019841145991402124,
       2.75516291724042e-06, -2.4917466240452868e-08, 1.446608995457697e-10)


def poly(coefs, t):
    total = jnp.full_like(t, coefs[-1])
    for c in coefs[-2::-1]:
        total = total * t + c
    return total


def butterflies(values):
    values = list(values)
    step = 1
    while step < len(values):
        for i in range(len(values)):
            if not i & step:
                u, v = values[i], values[i + step]
                values[i], values[i + step] = u + v, u - v
        step *= 2
    return values


def signs(count, dtype):
    rank = lax.broadcasted_iota(jnp.int32, (count, count), 0) & lax.broadcasted_iota(jnp.int32, (count, count), 1)
    parity = rank
    shift = 1
    while shift < count:
        parity = parity ^ (parity >> shift)
        shift *= 2
    return (1 - 2 * (parity & 1)).astype(dtype)


def split(x, axis):
    high = x.astype(jnp.bfloat16)
    low = (x - high.astype(jnp.float32)).astype(jnp.bfloat16)
    return jnp.concatenate([high, low], axis=axis)


def tile_turn(x, right, left):
    y = jnp.dot(split(x, 1), right, preferred_element_type=jnp.float32)
    return jnp.dot(left, split(y, 0), preferred_element_type=jnp.float32)


def trig(x, scale):
    t = x * x
    return poly(COS, t) * scale, x * poly(SIN, t) * scale


def rotate(real, imag, c, s):
    return real * c + imag * s, imag * c - real * s


def pick_kernel(slabs, size, place_ref, wave_ref, level_ref, angle_ref, *refs):
    outs, sems = refs[:-1], refs[-1]
    mine = place_ref[0] // size
    pairs = list(zip((wave_ref, level_ref, angle_ref), outs))
    pairs += [(level_ref.at[pl.ds((mine ^ m) * size, size)], outs[m + 2]) for m in range(1, slabs)]
    copies = [pltpu.make_async_copy(*pair, sems.at[k]) for k, pair in enumerate(pairs)]
    for copy in copies:
        copy.start()
    for copy in copies:
        copy.wait()


def first_kernel(slots, part, scale, wave_ref, level_ref, angle_ref, right_ref, left_ref, out_ref, held):
    lanes = wave_ref.shape[2]
    block = left_ref.shape[0]
    groups, per = len(slots) * part // block, block // part
    right, left = right_ref[...], left_ref[...]
    angle = jnp.broadcast_to(angle_ref[0:1, :], (block, lanes))
    for g in range(groups):
        rows = slice(g * block, (g + 1) * block)
        c, s = trig(angle * level_ref[rows, :], scale)
        for p, x in enumerate(rotate(wave_ref[0, rows, :], wave_ref[1, rows, :], c, s)):
            held[p, rows, :] = tile_turn(x, right, left)
    for p in range(2):
        for tile in range(block // 8):
            values = butterflies([held[p, g * block + tile * 8:g * block + tile * 8 + 8, :] for g in range(groups)])
            k, row = tile * 8 // part, tile * 8 % part
            for g, value in enumerate(values):
                out_ref[slots[g * per + k], p, row:row + 8, :] = value


def deal_kernel(slabs, size, place_ref, *refs):
    mine = place_ref[0] % size
    for k in range(size):
        for m in range(slabs):
            refs[slabs + k][m] = refs[m][mine ^ k]


def trig_kernel(slabs, size, scale, place_ref, angle_ref, *refs):
    level_refs, cos_ref, sin_ref = refs[:size], refs[size], refs[size + 1]
    angle = jnp.broadcast_to(angle_ref[1:2, :], cos_ref.shape[1:])
    for k in range(size):
        for m in range(slabs):
            whose = place_ref[0] ^ (m * size + k)
            cos_ref[whose], sin_ref[whose] = trig(angle * level_refs[k][m], scale)


def turn_devices(slabs, size, slots, tiles, seen_ref, cos_ref, sin_ref, held):
    for tile in tiles:
        rows = slice(tile * 8, tile * 8 + 8)
        for z in range(slabs):
            for p in range(2):
                values = butterflies([seen_ref[slots[z * size + q], p, rows, :] for q in range(size)])
                for q, value in enumerate(values):
                    held[z * size + q, p, rows, :] = value
        for q in range(size):
            real, imag = (butterflies([held[z * size + q, p, rows, :] for z in range(slabs)]) for p in range(2))
            for z in range(slabs):
                d = z * size + q
                real[z], imag[z] = rotate(real[z], imag[z], cos_ref[d, rows, :], sin_ref[d, rows, :])
            for p, values in enumerate((real, imag)):
                for z, value in enumerate(butterflies(values)):
                    held[z * size + q, p, rows, :] = value


def few_kernel(slabs, size, slots, place_ref, seen_ref, cos_ref, sin_ref, *refs):
    outs, held = refs[:slabs], refs[slabs]
    count = outs[0].shape[2] // 8
    turn_devices(slabs, size, slots, range(count), seen_ref, cos_ref, sin_ref, held)
    mine = place_ref[0] // size
    for m in range(slabs):
        for p in range(2):
            for tile in range(count):
                rows = slice(tile * 8, tile * 8 + 8)
                values = butterflies([held[(mine ^ m) * size + q, p, rows, :] for q in range(size)])
                for q, value in enumerate(values):
                    outs[m][q, p, rows, :] = value


def most_kernel(slabs, size, slots, seen_ref, cos_ref, sin_ref, right_ref, left_ref, out_ref, held):
    part, lanes = seen_ref.shape[2:]
    devices = slabs * size
    start = (part - out_ref.shape[2]) // 8
    turn_devices(slabs, size, slots, range(start, part // 8), seen_ref, cos_ref, sin_ref, held)
    right, left = right_ref[...], left_ref[...]
    step = left.shape[0] // 8
    for tile in range(start, part // 8):
        rows = slice(tile * 8, tile * 8 + 8)
        for p in range(2):
            for z in range(slabs):
                values = butterflies([held[z * size + q, p, rows, :] for q in range(size)])
                for q, value in enumerate(values):
                    held[z * size + q, p, rows, :] = value
            for d in range(0, devices, step):
                x = held[d:d + step, p, rows, :].reshape(step * 8, lanes)
                out_ref[d:d + step, p, (tile - start) * 8:(tile - start) * 8 + 8, :] = tile_turn(x, right, left).reshape(step, 8, lanes)


def gather_kernel(slabs, size, place_ref, right_ref, left_ref, *refs):
    parts, out_ref, held = refs[:size], refs[size], refs[size + 1]
    for k in range(size):
        for m in range(slabs):
            held[place_ref[0] ^ (m * size + k)] = parts[k][m]
    right, left = right_ref[...], left_ref[...]
    step = left.shape[0] // 8
    for p in range(2):
        for d in range(0, slabs * size, step):
            for row in range(0, held.shape[2], 8):
                x = held[d:d + step, p, row:row + 8, :].reshape(step * 8, held.shape[3])
                out_ref[d:d + step, p, row:row + 8, :] = tile_turn(x, right, left).reshape(step, 8, held.shape[3])


def last_kernel(devices, part, few_ref, most_ref, out_ref, held, done, sems):
    tiles = part // 8
    low = 4
    high = devices // low

    start = few_ref.shape[2] // 8

    def source(d, p, tile):
        ref, row = (few_ref, tile * 8) if tile < start else (most_ref, (tile - start) * 8)
        return ref[d, p, row:row + 8, :]

    copies = []
    for p in range(2):
        for k in range(low):
            for tile in range(tiles):
                values = butterflies([source(h * low + k, p, tile) for h in range(high)])
                for h, value in enumerate(values):
                    held[p, h, k * tiles + tile] = value
        for h in range(high):
            values = butterflies([held[p, h, i] for i in range(low * tiles)])
            for i, value in enumerate(values):
                done[p, (h * low * tiles + i) * 8:(h * low * tiles + i) * 8 + 8, :] = value
            rows = pl.ds(h * low * part, low * part)
            copies.append(pltpu.make_async_copy(done.at[p, rows], out_ref.at[p, rows], sems.at[p * high + h]))
            copies[-1].start()
    for copy in copies:
        copy.wait()


def near(x):
    return pltpu.with_memory_space_constraint(x, pltpu.VMEM)


def far(x):
    return pltpu.with_memory_space_constraint(x, pltpu.HBM)


def flat(*shape):
    return jax.ShapeDtypeStruct(shape, jnp.float32)


def held_shape(*shape):
    return pltpu.VMEM(shape, jnp.float32)


def swap(x, axes, devices, mask):
    return lax.ppermute(x, axes, [(i, i ^ mask) for i in range(devices)])


FEW = 16
PARAMS = pltpu.CompilerParams(vmem_limit_bytes=16 * 2**20)
SCALAR = pl.BlockSpec(memory_space=pltpu.SMEM)
WHOLE = pl.BlockSpec(memory_space=pltpu.VMEM)
FAR = pl.BlockSpec(memory_space=pltpu.HBM)


def low_masks(size, core):
    far = sorted((k for k in range(1, size) if not k & core), key=lambda k: (k.bit_count(), -k))
    return [*far, *(k | core for k in far), core]


def device_order(devices, core):
    low, high = core.bit_length() - 1, devices.bit_length() - 1
    bits = [high - 1, *range(low - 1, -1, -1), low + 1, *range(high - 2, low + 1, -1), low]
    order = [sum((rank >> (high - 1 - i) & 1) << bit for i, bit in enumerate(bits)) for rank in range(devices)]
    return order, [order.index(d) for d in range(devices)]


def kernel_call(kernel, in_specs, out_shape, scratch=(), out_specs=None):
    count = len(out_shape) if isinstance(out_shape, list) else 0
    return pl.pallas_call(
        kernel,
        in_specs=in_specs,
        out_specs=out_specs or ([WHOLE] * count if count else WHOLE),
        out_shape=out_shape,
        scratch_shapes=list(scratch),
        compiler_params=PARAMS,
    )


def body_fast(axes, devices, slabs, core, wave, levels, angles):
    blocks, rows, lanes = levels.shape
    total = blocks * rows
    part = total // devices
    size = devices // slabs
    count = FEW
    scale = float(devices * total * lanes) ** -0.5
    order, slots = device_order(devices, core)
    place = lax.axis_index(axes).astype(jnp.int32).reshape(1)
    wave = wave.reshape(2, total, lanes)
    levels = levels.reshape(devices, part, lanes)
    sign = signs(lanes, jnp.bfloat16)
    right = jnp.concatenate([sign, sign], axis=0)
    full = signs(128, jnp.bfloat16)
    rank = jnp.arange(128)
    small = jnp.where(rank[:, None] // 8 == rank[None, :] // 8, jnp.tile(signs(8, jnp.bfloat16), (16, 16)), 0)
    left = jnp.concatenate([full, full], axis=1)
    left_small = jnp.concatenate([small, small], axis=1)

    wave, levels, angles, *picked = kernel_call(
        functools.partial(pick_kernel, slabs, size), [SCALAR] + [FAR] * 3,
        [held_shape(*x.shape) for x in (wave, levels, angles)] + [held_shape(size, part, lanes)] * (slabs - 1),
        [pltpu.SemaphoreType.DMA((slabs + 2,))],
    )(place, far(wave), far(levels), far(angles))
    own = lax.dynamic_slice_in_dim(levels, place[0] // size * size, size, 0)
    mine = [own]
    for m in range(1, slabs):
        mine.append(swap(picked[m - 1], axes, devices, m * size))
    sent = kernel_call(
        functools.partial(first_kernel, slots, part, scale), [WHOLE] * 5,
        flat(devices, 2, part, lanes), [held_shape(2, total, lanes)],
    )(near(wave), near(levels.reshape(total, lanes)), near(angles), right, left)
    seen = lax.all_to_all(sent, axes, 0, 0, tiled=True, axis_index_groups=[order])
    dealt = kernel_call(
        functools.partial(deal_kernel, slabs, size), [SCALAR] + [WHOLE] * slabs,
        [held_shape(slabs, part, lanes)] * size,
    )(place, *map(near, mine))
    dealt = [dealt[0]] + [swap(dealt[k], axes, devices, k) for k in range(1, size)]
    cos, sin = kernel_call(
        functools.partial(trig_kernel, slabs, size, scale), [SCALAR] + [WHOLE] * (1 + size),
        [held_shape(devices, part, lanes)] * 2,
    )(place, near(angles), *map(near, dealt))

    seen = near(seen)
    few = kernel_call(
        functools.partial(few_kernel, slabs, size, slots), [SCALAR] + [WHOLE] * 3,
        [held_shape(size, 2, count, lanes)] * slabs, [held_shape(devices, 2, count, lanes)],
    )(place, seen, cos, sin)
    few = [few[0], *few[1:]]
    for m in range(1, slabs):
        few[m] = swap(few[m], axes, devices, m * size)
    most = kernel_call(
        functools.partial(most_kernel, slabs, size, slots), [WHOLE] * 5,
        flat(devices, 2, part - count, lanes), [held_shape(devices, 2, part, lanes)],
    )(seen, cos, sin, right, left_small)
    most = lax.all_to_all(most, axes, 0, 0, tiled=True)
    few = kernel_call(
        functools.partial(deal_kernel, slabs, size), [SCALAR] + [WHOLE] * slabs,
        [held_shape(slabs, 2, count, lanes)] * size,
    )(place, *map(near, few))
    few = list(few)
    for k in low_masks(size, core):
        few[k] = swap(few[k], axes, devices, k)
    few = kernel_call(
        functools.partial(gather_kernel, slabs, size), [SCALAR] + [WHOLE] * (2 + size),
        held_shape(devices, 2, count, lanes), [held_shape(devices, 2, count, lanes)],
    )(place, right, left_small, *map(near, few))
    out = kernel_call(
        functools.partial(last_kernel, devices, part), [WHOLE] * 2, flat(2, total, lanes),
        [held_shape(2, devices // 4, part // 2, 8, lanes), held_shape(2, total, lanes), pltpu.SemaphoreType.DMA((devices // 2,))],
        FAR,
    )(near(few), near(most))
    return out.reshape(2, blocks, rows, lanes)


def walsh(values, dim):
    count = values.shape[dim]
    moved = jnp.tensordot(values, signs(count, jnp.float32), axes=([dim], [0]), precision=lax.Precision.HIGHEST)
    return jnp.moveaxis(moved, -1, dim) * count ** -0.5


def body_plain(axes, devices, wave, levels, angles):
    blocks, rows, lanes = levels.shape
    part = blocks * rows // devices
    values = wave.reshape(2, devices, part, lanes)
    levels = levels.reshape(devices, part, lanes)
    x = angles[0] * levels
    c, s = jnp.cos(x), jnp.sin(x)
    values = jnp.stack([values[0] * c + values[1] * s, values[1] * c - values[0] * s], axis=1)
    values = walsh(values, 0)
    values = lax.all_to_all(values, axes, 0, 0, tiled=True)
    levels = lax.all_to_all(levels, axes, 0, 0, tiled=True)
    for dim in (0, 2, 3):
        values = walsh(values, dim)
    x = angles[1] * levels
    c, s = jnp.cos(x), jnp.sin(x)
    values = jnp.stack([values[:, 0] * c + values[:, 1] * s, values[:, 1] * c - values[:, 0] * s], axis=1)
    for dim in (0, 2, 3):
        values = walsh(values, dim)
    values = lax.all_to_all(values, axes, 0, 0, tiled=True)
    values = walsh(values, 0)
    return jnp.moveaxis(values, 1, 0).reshape(wave.shape)


def solution(mesh):
    axes = ("qa", "qb")
    devices = mesh.shape["qa"] * mesh.shape["qb"]

    def body(wave, levels, angles):
        total = levels.shape[0] * levels.shape[1]
        part = total // devices
        fast = part % 16 == 0 and 128 % part == 0 and total % 128 == 0 and devices % 16 == 0
        slabs = mesh.shape["qa"] // 4
        if fast and slabs > 1:
            return body_fast(axes, devices, slabs, mesh.shape["qb"], wave, levels, angles)
        return body_plain(axes, devices, wave, levels, angles)

    in_specs = (P(None, axes, None, None), P(axes, None, None), P())
    return jax.shard_map(body, mesh=mesh, in_specs=in_specs, out_specs=in_specs[0], check_vma=False)
```

```python
import functools

import jax
import jax.numpy as jnp
from jax import lax
from jax.experimental import pallas as pl
from jax.experimental.pallas import tpu as pltpu
from jax.sharding import PartitionSpec as P


COS = (0.99999999952702, -0.49999999256864713, 0.04166664759095227, -0.0013888705067900038,
       2.4793136218611696e-05, -2.735711629719697e-07, 1.8502809653875554e-09)
SIN = (0.9999999999681006, -0.16666666616558576, 0.008333332047516205, -0.00019841145991402124,
       2.75516291724042e-06, -2.4917466240452868e-08, 1.446608995457697e-10)


def poly(coefs, t):
    total = jnp.full_like(t, coefs[-1])
    for c in coefs[-2::-1]:
        total = total * t + c
    return total


def butterflies(values):
    values = list(values)
    step = 1
    while step < len(values):
        for i in range(len(values)):
            if not i & step:
                u, v = values[i], values[i + step]
                values[i], values[i + step] = u + v, u - v
        step *= 2
    return values


def signs(count, dtype):
    rank = lax.broadcasted_iota(jnp.int32, (count, count), 0) & lax.broadcasted_iota(jnp.int32, (count, count), 1)
    parity = rank
    shift = 1
    while shift < count:
        parity = parity ^ (parity >> shift)
        shift *= 2
    return (1 - 2 * (parity & 1)).astype(dtype)


def split(x, axis):
    high = x.astype(jnp.bfloat16)
    low = (x - high.astype(jnp.float32)).astype(jnp.bfloat16)
    return jnp.concatenate([high, low], axis=axis)


def tile_turn(x, right, left):
    y = jnp.dot(split(x, 1), right, preferred_element_type=jnp.float32)
    return jnp.dot(left, split(y, 0), preferred_element_type=jnp.float32)


def trig(x, scale):
    t = x * x
    return poly(COS, t) * scale, x * poly(SIN, t) * scale


def rotate(real, imag, c, s):
    return real * c + imag * s, imag * c - real * s


def pick_kernel(slabs, size, place_ref, wave_ref, level_ref, angle_ref, *refs):
    outs, sems = refs[:-1], refs[-1]
    mine = place_ref[0] // size
    pairs = list(zip((wave_ref, level_ref, angle_ref), outs))
    pairs += [(level_ref.at[pl.ds((mine ^ m) * size, size)], outs[m + 2]) for m in range(1, slabs)]
    copies = [pltpu.make_async_copy(*pair, sems.at[k]) for k, pair in enumerate(pairs)]
    for copy in copies:
        copy.start()
    for copy in copies:
        copy.wait()


def first_kernel(slots, part, scale, wave_ref, level_ref, angle_ref, right_ref, left_ref, out_ref, held):
    lanes = wave_ref.shape[2]
    block = left_ref.shape[0]
    groups, per = len(slots) * part // block, block // part
    right, left = right_ref[...], left_ref[...]
    angle = jnp.broadcast_to(angle_ref[0:1, :], (block, lanes))
    for g in range(groups):
        rows = slice(g * block, (g + 1) * block)
        c, s = trig(angle * level_ref[rows, :], scale)
        for p, x in enumerate(rotate(wave_ref[0, rows, :], wave_ref[1, rows, :], c, s)):
            held[p, rows, :] = tile_turn(x, right, left)
    for p in range(2):
        for tile in range(block // 8):
            values = butterflies([held[p, g * block + tile * 8:g * block + tile * 8 + 8, :] for g in range(groups)])
            k, row = tile * 8 // part, tile * 8 % part
            for g, value in enumerate(values):
                out_ref[slots[g * per + k], p, row:row + 8, :] = value


def deal_kernel(slabs, size, place_ref, *refs):
    mine = place_ref[0] % size
    for k in range(size):
        for m in range(slabs):
            refs[slabs + k][m] = refs[m][mine ^ k]


def trig_kernel(slabs, size, scale, place_ref, angle_ref, *refs):
    level_refs, cos_ref, sin_ref = refs[:size], refs[size], refs[size + 1]
    angle = jnp.broadcast_to(angle_ref[1:2, :], cos_ref.shape[1:])
    for k in range(size):
        for m in range(slabs):
            whose = place_ref[0] ^ (m * size + k)
            cos_ref[whose], sin_ref[whose] = trig(angle * level_refs[k][m], scale)


def turn_devices(slabs, size, slots, tiles, seen_ref, cos_ref, sin_ref, held):
    for tile in tiles:
        rows = slice(tile * 8, tile * 8 + 8)
        for z in range(slabs):
            for p in range(2):
                values = butterflies([seen_ref[slots[z * size + q], p, rows, :] for q in range(size)])
                for q, value in enumerate(values):
                    held[z * size + q, p, rows, :] = value
        for q in range(size):
            real, imag = (butterflies([held[z * size + q, p, rows, :] for z in range(slabs)]) for p in range(2))
            for z in range(slabs):
                d = z * size + q
                real[z], imag[z] = rotate(real[z], imag[z], cos_ref[d, rows, :], sin_ref[d, rows, :])
            for p, values in enumerate((real, imag)):
                for z, value in enumerate(butterflies(values)):
                    held[z * size + q, p, rows, :] = value


def few_kernel(slabs, size, slots, place_ref, seen_ref, cos_ref, sin_ref, *refs):
    outs, held = refs[:slabs], refs[slabs]
    count = outs[0].shape[2] // 8
    turn_devices(slabs, size, slots, range(count), seen_ref, cos_ref, sin_ref, held)
    mine = place_ref[0] // size
    for m in range(slabs):
        for p in range(2):
            for tile in range(count):
                rows = slice(tile * 8, tile * 8 + 8)
                values = butterflies([held[(mine ^ m) * size + q, p, rows, :] for q in range(size)])
                for q, value in enumerate(values):
                    outs[m][q, p, rows, :] = value


def most_kernel(slabs, size, slots, seen_ref, cos_ref, sin_ref, right_ref, left_ref, out_ref, held):
    part, lanes = seen_ref.shape[2:]
    devices = slabs * size
    start = (part - out_ref.shape[2]) // 8
    turn_devices(slabs, size, slots, range(start, part // 8), seen_ref, cos_ref, sin_ref, held)
    right, left = right_ref[...], left_ref[...]
    step = left.shape[0] // 8
    for tile in range(start, part // 8):
        rows = slice(tile * 8, tile * 8 + 8)
        for p in range(2):
            for z in range(slabs):
                values = butterflies([held[z * size + q, p, rows, :] for q in range(size)])
                for q, value in enumerate(values):
                    held[z * size + q, p, rows, :] = value
            for d in range(0, devices, step):
                x = held[d:d + step, p, rows, :].reshape(step * 8, lanes)
                out_ref[d:d + step, p, (tile - start) * 8:(tile - start) * 8 + 8, :] = tile_turn(x, right, left).reshape(step, 8, lanes)


def gather_kernel(slabs, size, place_ref, right_ref, left_ref, *refs):
    parts, out_ref, held = refs[:size], refs[size], refs[size + 1]
    for k in range(size):
        for m in range(slabs):
            held[place_ref[0] ^ (m * size + k)] = parts[k][m]
    right, left = right_ref[...], left_ref[...]
    step = left.shape[0] // 8
    for p in range(2):
        for d in range(0, slabs * size, step):
            for row in range(0, held.shape[2], 8):
                x = held[d:d + step, p, row:row + 8, :].reshape(step * 8, held.shape[3])
                out_ref[d:d + step, p, row:row + 8, :] = tile_turn(x, right, left).reshape(step, 8, held.shape[3])


def last_kernel(devices, part, few_ref, most_ref, out_ref, held, done, sems):
    tiles = part // 8
    low = 8
    high = devices // low

    start = few_ref.shape[2] // 8

    def source(d, p, tile):
        ref, row = (few_ref, tile * 8) if tile < start else (most_ref, (tile - start) * 8)
        return ref[d, p, row:row + 8, :]

    copies = []
    for p in range(2):
        for k in range(low):
            for tile in range(tiles):
                values = butterflies([source(h * low + k, p, tile) for h in range(high)])
                for h, value in enumerate(values):
                    held[p, h, k * tiles + tile] = value
        for h in range(high):
            values = butterflies([held[p, h, i] for i in range(low * tiles)])
            for i, value in enumerate(values):
                done[p, (h * low * tiles + i) * 8:(h * low * tiles + i) * 8 + 8, :] = value
            rows = pl.ds(h * low * part, low * part)
            copies.append(pltpu.make_async_copy(done.at[p, rows], out_ref.at[p, rows], sems.at[p * high + h]))
            copies[-1].start()
    for copy in copies:
        copy.wait()


def near(x):
    return pltpu.with_memory_space_constraint(x, pltpu.VMEM)


def far(x):
    return pltpu.with_memory_space_constraint(x, pltpu.HBM)


def flat(*shape):
    return jax.ShapeDtypeStruct(shape, jnp.float32)


def held_shape(*shape):
    return pltpu.VMEM(shape, jnp.float32)


def swap(x, axes, devices, mask):
    return lax.ppermute(x, axes, [(i, i ^ mask) for i in range(devices)])


FEW = 16
PARAMS = pltpu.CompilerParams(vmem_limit_bytes=16 * 2**20)
SCALAR = pl.BlockSpec(memory_space=pltpu.SMEM)
WHOLE = pl.BlockSpec(memory_space=pltpu.VMEM)
FAR = pl.BlockSpec(memory_space=pltpu.HBM)


def low_masks(size, core):
    far = sorted((k for k in range(1, size) if not k & core), key=lambda k: (k.bit_count(), -k))
    return [*far, *(k | core for k in far), core]


def device_order(devices, core):
    low, high = core.bit_length() - 1, devices.bit_length() - 1
    bits = [high - 1, low + 1, *range(low - 1, -1, -1), *range(high - 2, low + 1, -1), low]
    order = [sum((rank >> (high - 1 - i) & 1) << bit for i, bit in enumerate(bits)) for rank in range(devices)]
    return order, [order.index(d) for d in range(devices)]


def kernel_call(kernel, in_specs, out_shape, scratch=(), out_specs=None):
    count = len(out_shape) if isinstance(out_shape, list) else 0
    return pl.pallas_call(
        kernel,
        in_specs=in_specs,
        out_specs=out_specs or ([WHOLE] * count if count else WHOLE),
        out_shape=out_shape,
        scratch_shapes=list(scratch),
        compiler_params=PARAMS,
    )


def body_fast(axes, devices, slabs, core, wave, levels, angles):
    blocks, rows, lanes = levels.shape
    total = blocks * rows
    part = total // devices
    size = devices // slabs
    count = FEW
    scale = float(devices * total * lanes) ** -0.5
    order, slots = device_order(devices, core)
    place = lax.axis_index(axes).astype(jnp.int32).reshape(1)
    wave = wave.reshape(2, total, lanes)
    levels = levels.reshape(devices, part, lanes)
    sign = signs(lanes, jnp.bfloat16)
    right = jnp.concatenate([sign, sign], axis=0)
    full = signs(128, jnp.bfloat16)
    rank = jnp.arange(128)
    small = jnp.where(rank[:, None] // 8 == rank[None, :] // 8, jnp.tile(signs(8, jnp.bfloat16), (16, 16)), 0)
    left = jnp.concatenate([full, full], axis=1)
    left_small = jnp.concatenate([small, small], axis=1)

    wave, levels, angles, *picked = kernel_call(
        functools.partial(pick_kernel, slabs, size), [SCALAR] + [FAR] * 3,
        [held_shape(*x.shape) for x in (wave, levels, angles)] + [held_shape(size, part, lanes)] * (slabs - 1),
        [pltpu.SemaphoreType.DMA((slabs + 2,))],
    )(place, far(wave), far(levels), far(angles))
    own = lax.dynamic_slice_in_dim(levels, place[0] // size * size, size, 0)
    mine = [own]
    for m in range(1, slabs):
        mine.append(swap(picked[m - 1], axes, devices, m * size))
    sent = kernel_call(
        functools.partial(first_kernel, slots, part, scale), [WHOLE] * 5,
        flat(devices, 2, part, lanes), [held_shape(2, total, lanes)],
    )(near(wave), near(levels.reshape(total, lanes)), near(angles), right, left)
    seen = lax.all_to_all(sent, axes, 0, 0, tiled=True, axis_index_groups=[order])
    dealt = kernel_call(
        functools.partial(deal_kernel, slabs, size), [SCALAR] + [WHOLE] * slabs,
        [held_shape(slabs, part, lanes)] * size,
    )(place, *map(near, mine))
    dealt = [dealt[0]] + [swap(dealt[k], axes, devices, k) for k in range(1, size)]
    cos, sin = kernel_call(
        functools.partial(trig_kernel, slabs, size, scale), [SCALAR] + [WHOLE] * (1 + size),
        [held_shape(devices, part, lanes)] * 2,
    )(place, near(angles), *map(near, dealt))

    seen = near(seen)
    few = kernel_call(
        functools.partial(few_kernel, slabs, size, slots), [SCALAR] + [WHOLE] * 3,
        [held_shape(size, 2, count, lanes)] * slabs, [held_shape(devices, 2, count, lanes)],
    )(place, seen, cos, sin)
    few = [few[0], *few[1:]]
    for m in range(1, slabs):
        few[m] = swap(few[m], axes, devices, m * size)
    most = kernel_call(
        functools.partial(most_kernel, slabs, size, slots), [WHOLE] * 5,
        flat(devices, 2, part - count, lanes), [held_shape(devices, 2, part, lanes)],
    )(seen, cos, sin, right, left_small)
    most = lax.all_to_all(most, axes, 0, 0, tiled=True)
    few = kernel_call(
        functools.partial(deal_kernel, slabs, size), [SCALAR] + [WHOLE] * slabs,
        [held_shape(slabs, 2, count, lanes)] * size,
    )(place, *map(near, few))
    few = list(few)
    for k in low_masks(size, core):
        few[k] = swap(few[k], axes, devices, k)
    few = kernel_call(
        functools.partial(gather_kernel, slabs, size), [SCALAR] + [WHOLE] * (2 + size),
        held_shape(devices, 2, count, lanes), [held_shape(devices, 2, count, lanes)],
    )(place, right, left_small, *map(near, few))
    out = kernel_call(
        functools.partial(last_kernel, devices, part), [WHOLE] * 2, flat(2, total, lanes),
        [held_shape(2, devices // 8, part * 8 // 8, 8, lanes), held_shape(2, total, lanes), pltpu.SemaphoreType.DMA((2 * devices // 8,))],
        FAR,
    )(near(few), near(most))
    return out.reshape(2, blocks, rows, lanes)


def walsh(values, dim):
    count = values.shape[dim]
    moved = jnp.tensordot(values, signs(count, jnp.float32), axes=([dim], [0]), precision=lax.Precision.HIGHEST)
    return jnp.moveaxis(moved, -1, dim) * count ** -0.5


def body_plain(axes, devices, wave, levels, angles):
    blocks, rows, lanes = levels.shape
    part = blocks * rows // devices
    values = wave.reshape(2, devices, part, lanes)
    levels = levels.reshape(devices, part, lanes)
    x = angles[0] * levels
    c, s = jnp.cos(x), jnp.sin(x)
    values = jnp.stack([values[0] * c + values[1] * s, values[1] * c - values[0] * s], axis=1)
    values = walsh(values, 0)
    values = lax.all_to_all(values, axes, 0, 0, tiled=True)
    levels = lax.all_to_all(levels, axes, 0, 0, tiled=True)
    for dim in (0, 2, 3):
        values = walsh(values, dim)
    x = angles[1] * levels
    c, s = jnp.cos(x), jnp.sin(x)
    values = jnp.stack([values[:, 0] * c + values[:, 1] * s, values[:, 1] * c - values[:, 0] * s], axis=1)
    for dim in (0, 2, 3):
        values = walsh(values, dim)
    values = lax.all_to_all(values, axes, 0, 0, tiled=True)
    values = walsh(values, 0)
    return jnp.moveaxis(values, 1, 0).reshape(wave.shape)


def solution(mesh):
    axes = ("qa", "qb")
    devices = mesh.shape["qa"] * mesh.shape["qb"]

    def body(wave, levels, angles):
        total = levels.shape[0] * levels.shape[1]
        part = total // devices
        fast = part % 16 == 0 and 128 % part == 0 and total % 128 == 0 and devices % 16 == 0
        slabs = mesh.shape["qa"] // 4
        if fast and slabs > 1:
            return body_fast(axes, devices, slabs, mesh.shape["qb"], wave, levels, angles)
        return body_plain(axes, devices, wave, levels, angles)

    in_specs = (P(None, axes, None, None), P(axes, None, None), P())
    return jax.shard_map(body, mesh=mesh, in_specs=in_specs, out_specs=in_specs[0], check_vma=False)
```

```python
import functools

import jax
import jax.numpy as jnp
from jax import lax
from jax.experimental import pallas as pl
from jax.experimental.pallas import tpu as pltpu
from jax.sharding import PartitionSpec as P


COS = (0.99999999952702, -0.49999999256864713, 0.04166664759095227, -0.0013888705067900038,
       2.4793136218611696e-05, -2.735711629719697e-07, 1.8502809653875554e-09)
SIN = (0.9999999999681006, -0.16666666616558576, 0.008333332047516205, -0.00019841145991402124,
       2.75516291724042e-06, -2.4917466240452868e-08, 1.446608995457697e-10)


def poly(coefs, t):
    total = jnp.full_like(t, coefs[-1])
    for c in coefs[-2::-1]:
        total = total * t + c
    return total


def butterflies(values):
    values = list(values)
    step = 1
    while step < len(values):
        for i in range(len(values)):
            if not i & step:
                u, v = values[i], values[i + step]
                values[i], values[i + step] = u + v, u - v
        step *= 2
    return values


def signs(count, dtype):
    rank = lax.broadcasted_iota(jnp.int32, (count, count), 0) & lax.broadcasted_iota(jnp.int32, (count, count), 1)
    parity = rank
    shift = 1
    while shift < count:
        parity = parity ^ (parity >> shift)
        shift *= 2
    return (1 - 2 * (parity & 1)).astype(dtype)


def split(x, axis):
    high = x.astype(jnp.bfloat16)
    low = (x - high.astype(jnp.float32)).astype(jnp.bfloat16)
    return jnp.concatenate([high, low], axis=axis)


def tile_turn(x, right, left):
    y = jnp.dot(split(x, 1), right, preferred_element_type=jnp.float32)
    return jnp.dot(left, split(y, 0), preferred_element_type=jnp.float32)


def trig(x, scale):
    t = x * x
    return poly(COS, t) * scale, x * poly(SIN, t) * scale


def rotate(real, imag, c, s):
    return real * c + imag * s, imag * c - real * s


def pick_kernel(slabs, size, place_ref, wave_ref, level_ref, angle_ref, *refs):
    outs, sems = refs[:-1], refs[-1]
    mine = place_ref[0] // size
    pairs = list(zip((wave_ref, level_ref, angle_ref), outs))
    pairs += [(level_ref.at[pl.ds((mine ^ m) * size, size)], outs[m + 2]) for m in range(1, slabs)]
    copies = [pltpu.make_async_copy(*pair, sems.at[k]) for k, pair in enumerate(pairs)]
    for copy in copies:
        copy.start()
    for copy in copies:
        copy.wait()


def first_kernel(slots, part, scale, wave_ref, level_ref, angle_ref, right_ref, left_ref, out_ref, held, done, sems):
    lanes = wave_ref.shape[2]
    block = left_ref.shape[0]
    groups, per = len(slots) * part // block, block // part
    right, left = right_ref[...], left_ref[...]
    angle = jnp.broadcast_to(angle_ref[0:1, :], (block, lanes))
    for g in range(groups):
        rows = slice(g * block, (g + 1) * block)
        c, s = trig(angle * level_ref[rows, :], scale)
        held[0, rows, :], held[1, rows, :] = rotate(wave_ref[0, rows, :], wave_ref[1, rows, :], c, s)
    copies = []
    for p in range(2):
        for g in range(groups):
            rows = slice(g * block, (g + 1) * block)
            held[p, rows, :] = tile_turn(held[p, rows, :], right, left)
        for tile in range(block // 8):
            values = butterflies([held[p, g * block + tile * 8:g * block + tile * 8 + 8, :] for g in range(groups)])
            k, row = tile * 8 // part, tile * 8 % part
            for g, value in enumerate(values):
                done[slots[g * per + k], p, row:row + 8, :] = value
        copies.append(pltpu.make_async_copy(done.at[:, p], out_ref.at[:, p], sems.at[p]))
        copies[-1].start()
    for copy in copies:
        copy.wait()


def deal_kernel(slabs, size, place_ref, *refs):
    mine = place_ref[0] % size
    for k in range(size):
        for m in range(slabs):
            refs[slabs + k][m] = refs[m][mine ^ k]


def trig_kernel(slabs, size, scale, place_ref, angle_ref, *refs):
    level_refs, cos_ref, sin_ref = refs[:size], refs[size], refs[size + 1]
    angle = jnp.broadcast_to(angle_ref[1:2, :], cos_ref.shape[1:])
    for k in range(size):
        for m in range(slabs):
            whose = place_ref[0] ^ (m * size + k)
            cos_ref[whose], sin_ref[whose] = trig(angle * level_refs[k][m], scale)


def turn_devices(slabs, size, slots, tiles, seen_ref, cos_ref, sin_ref, held):
    for tile in tiles:
        rows = slice(tile * 8, tile * 8 + 8)
        for z in range(slabs):
            for p in range(2):
                values = butterflies([seen_ref[slots[z * size + q], p, rows, :] for q in range(size)])
                for q, value in enumerate(values):
                    held[z * size + q, p, rows, :] = value
        for q in range(size):
            real, imag = (butterflies([held[z * size + q, p, rows, :] for z in range(slabs)]) for p in range(2))
            for z in range(slabs):
                d = z * size + q
                real[z], imag[z] = rotate(real[z], imag[z], cos_ref[d, rows, :], sin_ref[d, rows, :])
            for p, values in enumerate((real, imag)):
                for z, value in enumerate(butterflies(values)):
                    held[z * size + q, p, rows, :] = value


def few_kernel(slabs, size, slots, place_ref, seen_ref, cos_ref, sin_ref, *refs):
    outs, held = refs[:slabs], refs[slabs]
    count = outs[0].shape[2] // 8
    turn_devices(slabs, size, slots, range(count), seen_ref, cos_ref, sin_ref, held)
    mine = place_ref[0] // size
    for m in range(slabs):
        for p in range(2):
            for tile in range(count):
                rows = slice(tile * 8, tile * 8 + 8)
                values = butterflies([held[(mine ^ m) * size + q, p, rows, :] for q in range(size)])
                for q, value in enumerate(values):
                    outs[m][q, p, rows, :] = value


def most_kernel(slabs, size, slots, seen_ref, cos_ref, sin_ref, right_ref, left_ref, out_ref, held):
    part, lanes = seen_ref.shape[2:]
    devices = slabs * size
    start = (part - out_ref.shape[2]) // 8
    turn_devices(slabs, size, slots, range(start, part // 8), seen_ref, cos_ref, sin_ref, held)
    right, left = right_ref[...], left_ref[...]
    step = left.shape[0] // 8
    for tile in range(start, part // 8):
        rows = slice(tile * 8, tile * 8 + 8)
        for p in range(2):
            for z in range(slabs):
                values = butterflies([held[z * size + q, p, rows, :] for q in range(size)])
                for q, value in enumerate(values):
                    held[z * size + q, p, rows, :] = value
            for d in range(0, devices, step):
                x = held[d:d + step, p, rows, :].reshape(step * 8, lanes)
                out_ref[d:d + step, p, (tile - start) * 8:(tile - start) * 8 + 8, :] = tile_turn(x, right, left).reshape(step, 8, lanes)


def gather_kernel(slabs, size, place_ref, right_ref, left_ref, *refs):
    parts, out_ref, held = refs[:size], refs[size], refs[size + 1]
    for k in range(size):
        for m in range(slabs):
            held[place_ref[0] ^ (m * size + k)] = parts[k][m]
    right, left = right_ref[...], left_ref[...]
    step = left.shape[0] // 8
    for p in range(2):
        for d in range(0, slabs * size, step):
            for row in range(0, held.shape[2], 8):
                x = held[d:d + step, p, row:row + 8, :].reshape(step * 8, held.shape[3])
                out_ref[d:d + step, p, row:row + 8, :] = tile_turn(x, right, left).reshape(step, 8, held.shape[3])


def last_kernel(devices, part, few_ref, most_ref, out_ref, held, done, sems):
    tiles = part // 8
    low = 8
    high = devices // low

    start = few_ref.shape[2] // 8

    def source(d, p, tile):
        ref, row = (few_ref, tile * 8) if tile < start else (most_ref, (tile - start) * 8)
        return ref[d, p, row:row + 8, :]

    copies = []
    for p in range(2):
        for k in range(low):
            for tile in range(tiles):
                values = butterflies([source(h * low + k, p, tile) for h in range(high)])
                for h, value in enumerate(values):
                    held[p, h, k * tiles + tile] = value
        for h in range(high):
            values = butterflies([held[p, h, i] for i in range(low * tiles)])
            for i, value in enumerate(values):
                done[p, (h * low * tiles + i) * 8:(h * low * tiles + i) * 8 + 8, :] = value
            rows = pl.ds(h * low * part, low * part)
            copies.append(pltpu.make_async_copy(done.at[p, rows], out_ref.at[p, rows], sems.at[p * high + h]))
            copies[-1].start()
    for copy in copies:
        copy.wait()


def near(x):
    return pltpu.with_memory_space_constraint(x, pltpu.VMEM)


def far(x):
    return pltpu.with_memory_space_constraint(x, pltpu.HBM)


def flat(*shape):
    return jax.ShapeDtypeStruct(shape, jnp.float32)


def held_shape(*shape):
    return pltpu.VMEM(shape, jnp.float32)


def swap(x, axes, devices, mask):
    return lax.ppermute(x, axes, [(i, i ^ mask) for i in range(devices)])


FEW = 16
PARAMS = pltpu.CompilerParams(vmem_limit_bytes=16 * 2**20)
SCALAR = pl.BlockSpec(memory_space=pltpu.SMEM)
WHOLE = pl.BlockSpec(memory_space=pltpu.VMEM)
FAR = pl.BlockSpec(memory_space=pltpu.HBM)


def low_masks(size, core):
    far = sorted((k for k in range(1, size) if not k & core), key=lambda k: (k.bit_count(), -k))
    return [*far, *(k | core for k in far), core]


def device_order(devices, core):
    low, high = core.bit_length() - 1, devices.bit_length() - 1
    bits = [high - 1, low + 1, *range(low - 1, -1, -1), *range(high - 2, low + 1, -1), low]
    order = [sum((rank >> (high - 1 - i) & 1) << bit for i, bit in enumerate(bits)) for rank in range(devices)]
    return order, [order.index(d) for d in range(devices)]


def kernel_call(kernel, in_specs, out_shape, scratch=(), out_specs=None):
    count = len(out_shape) if isinstance(out_shape, list) else 0
    return pl.pallas_call(
        kernel,
        in_specs=in_specs,
        out_specs=out_specs or ([WHOLE] * count if count else WHOLE),
        out_shape=out_shape,
        scratch_shapes=list(scratch),
        compiler_params=PARAMS,
    )


def body_fast(axes, devices, slabs, core, wave, levels, angles):
    blocks, rows, lanes = levels.shape
    total = blocks * rows
    part = total // devices
    size = devices // slabs
    count = FEW
    scale = float(devices * total * lanes) ** -0.5
    order, slots = device_order(devices, core)
    place = lax.axis_index(axes).astype(jnp.int32).reshape(1)
    wave = wave.reshape(2, total, lanes)
    levels = levels.reshape(devices, part, lanes)
    sign = signs(lanes, jnp.bfloat16)
    right = jnp.concatenate([sign, sign], axis=0)
    full = signs(128, jnp.bfloat16)
    rank = jnp.arange(128)
    small = jnp.where(rank[:, None] // 8 == rank[None, :] // 8, jnp.tile(signs(8, jnp.bfloat16), (16, 16)), 0)
    left = jnp.concatenate([full, full], axis=1)
    left_small = jnp.concatenate([small, small], axis=1)

    wave, levels, angles, *picked = kernel_call(
        functools.partial(pick_kernel, slabs, size), [SCALAR] + [FAR] * 3,
        [held_shape(*x.shape) for x in (wave, levels, angles)] + [held_shape(size, part, lanes)] * (slabs - 1),
        [pltpu.SemaphoreType.DMA((slabs + 2,))],
    )(place, far(wave), far(levels), far(angles))
    own = lax.dynamic_slice_in_dim(levels, place[0] // size * size, size, 0)
    mine = [own]
    for m in range(1, slabs):
        mine.append(swap(picked[m - 1], axes, devices, m * size))
    sent = kernel_call(
        functools.partial(first_kernel, slots, part, scale), [WHOLE] * 5,
        flat(devices, 2, part, lanes),
        [held_shape(2, total, lanes), held_shape(devices, 2, part, lanes), pltpu.SemaphoreType.DMA((2,))], FAR,
    )(near(wave), near(levels.reshape(total, lanes)), near(angles), right, left)
    seen = lax.all_to_all(sent, axes, 0, 0, tiled=True, axis_index_groups=[order])
    dealt = kernel_call(
        functools.partial(deal_kernel, slabs, size), [SCALAR] + [WHOLE] * slabs,
        [held_shape(slabs, part, lanes)] * size,
    )(place, *map(near, mine))
    dealt = list(dealt)
    for k in low_masks(size, core)[::-1]:
        dealt[k] = swap(dealt[k], axes, devices, k)
    cos, sin = kernel_call(
        functools.partial(trig_kernel, slabs, size, scale), [SCALAR] + [WHOLE] * (1 + size),
        [held_shape(devices, part, lanes)] * 2,
    )(place, near(angles), *map(near, dealt))

    seen = near(seen)
    few = kernel_call(
        functools.partial(few_kernel, slabs, size, slots), [SCALAR] + [WHOLE] * 3,
        [held_shape(size, 2, count, lanes)] * slabs, [held_shape(devices, 2, count, lanes)],
    )(place, seen, cos, sin)
    few = [few[0], *few[1:]]
    for m in range(1, slabs):
        few[m] = swap(few[m], axes, devices, m * size)
    most = kernel_call(
        functools.partial(most_kernel, slabs, size, slots), [WHOLE] * 5,
        flat(devices, 2, part - count, lanes), [held_shape(devices, 2, part, lanes)],
    )(seen, cos, sin, right, left_small)
    most = lax.all_to_all(most, axes, 0, 0, tiled=True)
    few = kernel_call(
        functools.partial(deal_kernel, slabs, size), [SCALAR] + [WHOLE] * slabs,
        [held_shape(slabs, 2, count, lanes)] * size,
    )(place, *map(near, few))
    few = list(few)
    for k in low_masks(size, core):
        few[k] = swap(few[k], axes, devices, k)
    few = kernel_call(
        functools.partial(gather_kernel, slabs, size), [SCALAR] + [WHOLE] * (2 + size),
        held_shape(devices, 2, count, lanes), [held_shape(devices, 2, count, lanes)],
    )(place, right, left_small, *map(near, few))
    out = kernel_call(
        functools.partial(last_kernel, devices, part), [WHOLE] * 2, flat(2, total, lanes),
        [held_shape(2, devices // 8, part * 8 // 8, 8, lanes), held_shape(2, total, lanes), pltpu.SemaphoreType.DMA((2 * devices // 8,))],
        FAR,
    )(near(few), near(most))
    return out.reshape(2, blocks, rows, lanes)


def walsh(values, dim):
    count = values.shape[dim]
    moved = jnp.tensordot(values, signs(count, jnp.float32), axes=([dim], [0]), precision=lax.Precision.HIGHEST)
    return jnp.moveaxis(moved, -1, dim) * count ** -0.5


def body_plain(axes, devices, wave, levels, angles):
    blocks, rows, lanes = levels.shape
    part = blocks * rows // devices
    values = wave.reshape(2, devices, part, lanes)
    levels = levels.reshape(devices, part, lanes)
    x = angles[0] * levels
    c, s = jnp.cos(x), jnp.sin(x)
    values = jnp.stack([values[0] * c + values[1] * s, values[1] * c - values[0] * s], axis=1)
    values = walsh(values, 0)
    values = lax.all_to_all(values, axes, 0, 0, tiled=True)
    levels = lax.all_to_all(levels, axes, 0, 0, tiled=True)
    for dim in (0, 2, 3):
        values = walsh(values, dim)
    x = angles[1] * levels
    c, s = jnp.cos(x), jnp.sin(x)
    values = jnp.stack([values[:, 0] * c + values[:, 1] * s, values[:, 1] * c - values[:, 0] * s], axis=1)
    for dim in (0, 2, 3):
        values = walsh(values, dim)
    values = lax.all_to_all(values, axes, 0, 0, tiled=True)
    values = walsh(values, 0)
    return jnp.moveaxis(values, 1, 0).reshape(wave.shape)


def solution(mesh):
    axes = ("qa", "qb")
    devices = mesh.shape["qa"] * mesh.shape["qb"]

    def body(wave, levels, angles):
        total = levels.shape[0] * levels.shape[1]
        part = total // devices
        fast = part % 16 == 0 and 128 % part == 0 and total % 128 == 0 and devices % 16 == 0
        slabs = mesh.shape["qa"] // 4
        if fast and slabs > 1:
            return body_fast(axes, devices, slabs, mesh.shape["qb"], wave, levels, angles)
        return body_plain(axes, devices, wave, levels, angles)

    in_specs = (P(None, axes, None, None), P(axes, None, None), P())
    return jax.shard_map(body, mesh=mesh, in_specs=in_specs, out_specs=in_specs[0], check_vma=False)
```

```python
import functools

import jax
import jax.numpy as jnp
from jax import lax
from jax.experimental import pallas as pl
from jax.experimental.pallas import tpu as pltpu
from jax.sharding import PartitionSpec as P


COS = (0.99999999952702, -0.49999999256864713, 0.04166664759095227, -0.0013888705067900038,
       2.4793136218611696e-05, -2.735711629719697e-07, 1.8502809653875554e-09)
SIN = (0.9999999999681006, -0.16666666616558576, 0.008333332047516205, -0.00019841145991402124,
       2.75516291724042e-06, -2.4917466240452868e-08, 1.446608995457697e-10)


def poly(coefs, t):
    total = jnp.full_like(t, coefs[-1])
    for c in coefs[-2::-1]:
        total = total * t + c
    return total


def butterflies(values):
    values = list(values)
    step = 1
    while step < len(values):
        for i in range(len(values)):
            if not i & step:
                u, v = values[i], values[i + step]
                values[i], values[i + step] = u + v, u - v
        step *= 2
    return values


def signs(count, dtype):
    rank = lax.broadcasted_iota(jnp.int32, (count, count), 0) & lax.broadcasted_iota(jnp.int32, (count, count), 1)
    parity = rank
    shift = 1
    while shift < count:
        parity = parity ^ (parity >> shift)
        shift *= 2
    return (1 - 2 * (parity & 1)).astype(dtype)


def split(x, axis):
    high = x.astype(jnp.bfloat16)
    low = (x - high.astype(jnp.float32)).astype(jnp.bfloat16)
    return jnp.concatenate([high, low], axis=axis)


def tile_turn(x, right, left):
    y = jnp.dot(split(x, 1), right, preferred_element_type=jnp.float32)
    return jnp.dot(left, split(y, 0), preferred_element_type=jnp.float32)


def trig(x, scale):
    t = x * x
    return poly(COS, t) * scale, x * poly(SIN, t) * scale


def rotate(real, imag, c, s):
    return real * c + imag * s, imag * c - real * s


def pick_kernel(slabs, size, place_ref, wave_ref, level_ref, angle_ref, *refs):
    outs, sems = refs[:-1], refs[-1]
    mine = place_ref[0] // size
    pairs = list(zip((wave_ref, level_ref, angle_ref), outs))
    pairs += [(level_ref.at[pl.ds((mine ^ m) * size, size)], outs[m + 2]) for m in range(1, slabs)]
    copies = [pltpu.make_async_copy(*pair, sems.at[k]) for k, pair in enumerate(pairs)]
    for copy in copies:
        copy.start()
    for copy in copies:
        copy.wait()


def first_kernel(slots, part, scale, wave_ref, level_ref, angle_ref, right_ref, left_ref, out_ref, held, done, sems):
    lanes = wave_ref.shape[2]
    block = left_ref.shape[0]
    groups, per = len(slots) * part // block, block // part
    right, left = right_ref[...], left_ref[...]
    angle = jnp.broadcast_to(angle_ref[0:1, :], (block, lanes))
    for g in range(groups):
        rows = slice(g * block, (g + 1) * block)
        c, s = trig(angle * level_ref[rows, :], scale)
        held[0, rows, :], held[1, rows, :] = rotate(wave_ref[0, rows, :], wave_ref[1, rows, :], c, s)
    copies = []
    for p in range(2):
        for g in range(groups):
            rows = slice(g * block, (g + 1) * block)
            held[p, rows, :] = tile_turn(held[p, rows, :], right, left)
        for tile in range(block // 8):
            values = butterflies([held[p, g * block + tile * 8:g * block + tile * 8 + 8, :] for g in range(groups)])
            k, row = tile * 8 // part, tile * 8 % part
            for g, value in enumerate(values):
                done[slots[g * per + k], p, row:row + 8, :] = value
        copies.append(pltpu.make_async_copy(done.at[:, p], out_ref.at[:, p], sems.at[p]))
        copies[-1].start()
    for copy in copies:
        copy.wait()


def deal_kernel(slabs, size, place_ref, *refs):
    mine = place_ref[0] % size
    for k in range(size):
        for m in range(slabs):
            refs[slabs + k][m] = refs[m][mine ^ k]


def trig_kernel(slabs, size, scale, place_ref, angle_ref, *refs):
    level_refs, cos_ref, sin_ref = refs[:size], refs[size], refs[size + 1]
    angle = jnp.broadcast_to(angle_ref[1:2, :], cos_ref.shape[1:])
    for k in range(size):
        for m in range(slabs):
            whose = place_ref[0] ^ (m * size + k)
            cos_ref[whose], sin_ref[whose] = trig(angle * level_refs[k][m], scale)


def turn_devices(slabs, size, slots, tiles, seen_ref, cos_ref, sin_ref, held):
    for tile in tiles:
        rows = slice(tile * 8, tile * 8 + 8)
        for z in range(slabs):
            for p in range(2):
                values = butterflies([seen_ref[slots[z * size + q], p, rows, :] for q in range(size)])
                for q, value in enumerate(values):
                    held[z * size + q, p, rows, :] = value
        for q in range(size):
            real, imag = (butterflies([held[z * size + q, p, rows, :] for z in range(slabs)]) for p in range(2))
            for z in range(slabs):
                d = z * size + q
                real[z], imag[z] = rotate(real[z], imag[z], cos_ref[d, rows, :], sin_ref[d, rows, :])
            for p, values in enumerate((real, imag)):
                for z, value in enumerate(butterflies(values)):
                    held[z * size + q, p, rows, :] = value


def few_kernel(slabs, size, slots, place_ref, seen_ref, cos_ref, sin_ref, *refs):
    outs, held = refs[:slabs], refs[slabs]
    count = outs[0].shape[2] // 8
    turn_devices(slabs, size, slots, range(count), seen_ref, cos_ref, sin_ref, held)
    mine = place_ref[0] // size
    for m in range(slabs):
        for p in range(2):
            for tile in range(count):
                rows = slice(tile * 8, tile * 8 + 8)
                values = butterflies([held[(mine ^ m) * size + q, p, rows, :] for q in range(size)])
                for q, value in enumerate(values):
                    outs[m][q, p, rows, :] = value


def most_kernel(slabs, size, slots, seen_ref, cos_ref, sin_ref, right_ref, left_ref, out_ref, held):
    part, lanes = seen_ref.shape[2:]
    devices = slabs * size
    start = (part - out_ref.shape[2]) // 8
    turn_devices(slabs, size, slots, range(start, part // 8), seen_ref, cos_ref, sin_ref, held)
    right, left = right_ref[...], left_ref[...]
    step = left.shape[0] // 8
    for tile in range(start, part // 8):
        rows = slice(tile * 8, tile * 8 + 8)
        for p in range(2):
            for z in range(slabs):
                values = butterflies([held[z * size + q, p, rows, :] for q in range(size)])
                for q, value in enumerate(values):
                    held[z * size + q, p, rows, :] = value
            for d in range(0, devices, step):
                x = held[d:d + step, p, rows, :].reshape(step * 8, lanes)
                out_ref[d:d + step, p, (tile - start) * 8:(tile - start) * 8 + 8, :] = tile_turn(x, right, left).reshape(step, 8, lanes)


def gather_kernel(slabs, size, kinds, place_ref, right_ref, left_ref, *refs):
    parts, out_ref = refs[:len(kinds)], refs[-1]
    right, left = right_ref[...], left_ref[...]
    count, lanes = out_ref.shape[2:]
    step = left.shape[0] // (slabs * count)
    for p in range(2):
        for i in range(0, len(kinds), step):
            x = jnp.concatenate([part[:, p].reshape(slabs * count, lanes) for part in parts[i:i + step]], axis=0)
            y = tile_turn(x, right, left).reshape(step, slabs, count, lanes)
            for j in range(step):
                for m in range(slabs):
                    out_ref[place_ref[0] ^ (m * size + kinds[i + j]), p] = y[j, m]


def last_kernel(devices, part, few_ref, most_ref, out_ref, held, done, sems):
    tiles = part // 8
    low = 8
    high = devices // low

    start = few_ref.shape[2] // 8

    def source(d, p, tile):
        ref, row = (few_ref, tile * 8) if tile < start else (most_ref, (tile - start) * 8)
        return ref[d, p, row:row + 8, :]

    copies = []
    for p in range(2):
        for k in range(low):
            for tile in range(tiles):
                values = butterflies([source(h * low + k, p, tile) for h in range(high)])
                for h, value in enumerate(values):
                    held[p, h, k * tiles + tile] = value
        for h in range(high):
            values = butterflies([held[p, h, i] for i in range(low * tiles)])
            for i, value in enumerate(values):
                done[p, (h * low * tiles + i) * 8:(h * low * tiles + i) * 8 + 8, :] = value
            rows = pl.ds(h * low * part, low * part)
            copies.append(pltpu.make_async_copy(done.at[p, rows], out_ref.at[p, rows], sems.at[p * high + h]))
            copies[-1].start()
    for copy in copies:
        copy.wait()


def near(x):
    return pltpu.with_memory_space_constraint(x, pltpu.VMEM)


def far(x):
    return pltpu.with_memory_space_constraint(x, pltpu.HBM)


def flat(*shape):
    return jax.ShapeDtypeStruct(shape, jnp.float32)


def held_shape(*shape):
    return pltpu.VMEM(shape, jnp.float32)


def swap(x, axes, devices, mask):
    return lax.ppermute(x, axes, [(i, i ^ mask) for i in range(devices)])


FEW = 16
PARAMS = pltpu.CompilerParams(vmem_limit_bytes=16 * 2**20)
SCALAR = pl.BlockSpec(memory_space=pltpu.SMEM)
WHOLE = pl.BlockSpec(memory_space=pltpu.VMEM)
FAR = pl.BlockSpec(memory_space=pltpu.HBM)


def low_masks(size, core):
    far = sorted((k for k in range(1, size) if not k & core), key=lambda k: (k.bit_count(), -k))
    return [*far, *(k | core for k in far), core]


def device_order(devices, core):
    low, high = core.bit_length() - 1, devices.bit_length() - 1
    bits = [high - 1, low + 1, *range(low - 1, -1, -1), *range(high - 2, low + 1, -1), low]
    order = [sum((rank >> (high - 1 - i) & 1) << bit for i, bit in enumerate(bits)) for rank in range(devices)]
    return order, [order.index(d) for d in range(devices)]


def kernel_call(kernel, in_specs, out_shape, scratch=(), out_specs=None):
    count = len(out_shape) if isinstance(out_shape, list) else 0
    return pl.pallas_call(
        kernel,
        in_specs=in_specs,
        out_specs=out_specs or ([WHOLE] * count if count else WHOLE),
        out_shape=out_shape,
        scratch_shapes=list(scratch),
        compiler_params=PARAMS,
    )


def body_fast(axes, devices, slabs, core, wave, levels, angles):
    blocks, rows, lanes = levels.shape
    total = blocks * rows
    part = total // devices
    size = devices // slabs
    count = FEW
    scale = float(devices * total * lanes) ** -0.5
    order, slots = device_order(devices, core)
    place = lax.axis_index(axes).astype(jnp.int32).reshape(1)
    wave = wave.reshape(2, total, lanes)
    levels = levels.reshape(devices, part, lanes)
    sign = signs(lanes, jnp.bfloat16)
    right = jnp.concatenate([sign, sign], axis=0)
    full = signs(128, jnp.bfloat16)
    rank = jnp.arange(128)
    small = jnp.where(rank[:, None] // 8 == rank[None, :] // 8, jnp.tile(signs(8, jnp.bfloat16), (16, 16)), 0)
    left = jnp.concatenate([full, full], axis=1)
    left_small = jnp.concatenate([small, small], axis=1)

    wave, levels, angles, *picked = kernel_call(
        functools.partial(pick_kernel, slabs, size), [SCALAR] + [FAR] * 3,
        [held_shape(*x.shape) for x in (wave, levels, angles)] + [held_shape(size, part, lanes)] * (slabs - 1),
        [pltpu.SemaphoreType.DMA((slabs + 2,))],
    )(place, far(wave), far(levels), far(angles))
    own = lax.dynamic_slice_in_dim(levels, place[0] // size * size, size, 0)
    mine = [own]
    for m in range(1, slabs):
        mine.append(swap(picked[m - 1], axes, devices, m * size))
    sent = kernel_call(
        functools.partial(first_kernel, slots, part, scale), [WHOLE] * 5,
        flat(devices, 2, part, lanes),
        [held_shape(2, total, lanes), held_shape(devices, 2, part, lanes), pltpu.SemaphoreType.DMA((2,))], FAR,
    )(near(wave), near(levels.reshape(total, lanes)), near(angles), right, left)
    seen = lax.all_to_all(sent, axes, 0, 0, tiled=True, axis_index_groups=[order])
    dealt = kernel_call(
        functools.partial(deal_kernel, slabs, size), [SCALAR] + [WHOLE] * slabs,
        [held_shape(slabs, part, lanes)] * size,
    )(place, *map(near, mine))
    dealt = list(dealt)
    for k in low_masks(size, core)[::-1]:
        dealt[k] = swap(dealt[k], axes, devices, k)
    cos, sin = kernel_call(
        functools.partial(trig_kernel, slabs, size, scale), [SCALAR] + [WHOLE] * (1 + size),
        [held_shape(devices, part, lanes)] * 2,
    )(place, near(angles), *map(near, dealt))

    seen = near(seen)
    few = kernel_call(
        functools.partial(few_kernel, slabs, size, slots), [SCALAR] + [WHOLE] * 3,
        [held_shape(size, 2, count, lanes)] * slabs, [held_shape(devices, 2, count, lanes)],
    )(place, seen, cos, sin)
    few = [few[0], *few[1:]]
    for m in range(1, slabs):
        few[m] = swap(few[m], axes, devices, m * size)
    most = kernel_call(
        functools.partial(most_kernel, slabs, size, slots), [WHOLE] * 5,
        flat(devices, 2, part - count, lanes), [held_shape(devices, 2, part, lanes)],
    )(seen, cos, sin, right, left_small)
    most = lax.all_to_all(most, axes, 0, 0, tiled=True)
    few = kernel_call(
        functools.partial(deal_kernel, slabs, size), [SCALAR] + [WHOLE] * slabs,
        [held_shape(slabs, 2, count, lanes)] * size,
    )(place, *map(near, few))
    few = list(few)
    for k in low_masks(size, core):
        few[k] = swap(few[k], axes, devices, k)
    kinds = [0, *low_masks(size, core)]
    done = []
    for some in (kinds[:size // 2], kinds[size // 2:]):
        specs = [SCALAR] + [WHOLE] * (2 + len(some) + len(done))
        done = [pl.pallas_call(
            functools.partial(gather_kernel, slabs, size, some), in_specs=specs, out_specs=WHOLE,
            out_shape=held_shape(devices, 2, count, lanes), compiler_params=PARAMS,
            input_output_aliases={len(specs) - 1: 0} if done else {},
        )(place, right, left_small, *(near(few[k]) for k in some), *map(near, done))]
    few = done[0]
    out = kernel_call(
        functools.partial(last_kernel, devices, part), [WHOLE] * 2, flat(2, total, lanes),
        [held_shape(2, devices // 8, part * 8 // 8, 8, lanes), held_shape(2, total, lanes), pltpu.SemaphoreType.DMA((2 * devices // 8,))],
        FAR,
    )(near(few), near(most))
    return out.reshape(2, blocks, rows, lanes)


def walsh(values, dim):
    count = values.shape[dim]
    moved = jnp.tensordot(values, signs(count, jnp.float32), axes=([dim], [0]), precision=lax.Precision.HIGHEST)
    return jnp.moveaxis(moved, -1, dim) * count ** -0.5


def body_plain(axes, devices, wave, levels, angles):
    blocks, rows, lanes = levels.shape
    part = blocks * rows // devices
    values = wave.reshape(2, devices, part, lanes)
    levels = levels.reshape(devices, part, lanes)
    x = angles[0] * levels
    c, s = jnp.cos(x), jnp.sin(x)
    values = jnp.stack([values[0] * c + values[1] * s, values[1] * c - values[0] * s], axis=1)
    values = walsh(values, 0)
    values = lax.all_to_all(values, axes, 0, 0, tiled=True)
    levels = lax.all_to_all(levels, axes, 0, 0, tiled=True)
    for dim in (0, 2, 3):
        values = walsh(values, dim)
    x = angles[1] * levels
    c, s = jnp.cos(x), jnp.sin(x)
    values = jnp.stack([values[:, 0] * c + values[:, 1] * s, values[:, 1] * c - values[:, 0] * s], axis=1)
    for dim in (0, 2, 3):
        values = walsh(values, dim)
    values = lax.all_to_all(values, axes, 0, 0, tiled=True)
    values = walsh(values, 0)
    return jnp.moveaxis(values, 1, 0).reshape(wave.shape)


def solution(mesh):
    axes = ("qa", "qb")
    devices = mesh.shape["qa"] * mesh.shape["qb"]

    def body(wave, levels, angles):
        total = levels.shape[0] * levels.shape[1]
        part = total // devices
        fast = part % 16 == 0 and 128 % part == 0 and total % 128 == 0 and devices % 16 == 0
        slabs = mesh.shape["qa"] // 4
        if fast and slabs > 1:
            return body_fast(axes, devices, slabs, mesh.shape["qb"], wave, levels, angles)
        return body_plain(axes, devices, wave, levels, angles)

    in_specs = (P(None, axes, None, None), P(axes, None, None), P())
    return jax.shard_map(body, mesh=mesh, in_specs=in_specs, out_specs=in_specs[0], check_vma=False)
```
